32 devices in a mesh: dom: 32 (over z, y, x, core).
Axes of the slice: x: 2, y: 2, z: 4, core: 2. Of those that a mesh axis runs over, the one named last changes fastest.
Arguments:
- features: bfloat16 [524288, 256], P('dom'), may hold values from -48 to 48, as said below
- w_first: bfloat16 [1280, 256], replicated, may hold values from -0.15625 to 0.15625
- w_second: bfloat16 [1280, 256], replicated, may hold values from -0.15625 to 0.15625
- seed_owner: int32 [9216, 1], P('dom'), may hold values from 0 to 31; in each aligned block of 288 rows (0 to 287, 288 to 575, ...) at most 18 rows name the same one
- seed_row: int32 [9216], P('dom'), may hold values from 0 to 16383
- hop1_owner: int32 [36864, 1], P('dom'), may hold values from 0 to 31; in each aligned block of 1152 rows (0 to 1151, 1152 to 2303, ...) at most 72 rows name the same one
- hop1_row: int32 [36864], P('dom'), may hold values from 0 to 16383
- hop1_rel: int32 [36864], P('dom'), may hold values from 0 to 3
- hop2_owner: int32 [73728, 1], P('dom'), may hold values from 0 to 31; in each aligned block of 2304 rows (0 to 2303, 2304 to 4607, ...) at most 144 rows name the same one
- hop2_row: int32 [73728], P('dom'), may hold values from 0 to 16383
- hop2_rel: int32 [73728], P('dom'), may hold values from 0 to 3
- edge_mask: int32 [4096], P('dom'), may hold values 0 or 1
Outputs:
- edge_loss: float32 [4096], P('dom')
- mean_loss: float32 [], replicated
The draws below stay inside these ranges and needn't reach their ends.
Inputs may be any that keep to these rules, and one draw needn't show every extreme that they name: `features`: standard normal entries; in some draws each row is scaled by a factor up to 10. `seed_owner`: among the rows of one device no owner is named by more than 18 rows; some owner is named by exactly 18 in every draw. `hop1_owner`: among the rows of one device no owner is named by more than 72 rows; some owner is named by exactly 72 in every draw. `hop2_owner`: among the rows of one device no owner is named by more than 144 rows; some owner is named by exactly 144 in every draw.
All inputs are finite; a program needn't handle non-finite values. No bound on the sum of `edge_mask` on one device may be relied on, other than what follows from the above.
Results may differ from the reference program's by a relative error of at most 0.002.
Values may be sent and summed in bfloat16 or wider, within the bound.
No kernel may reach another device: no remote copies, remote signals or barrier semaphores. Data moves between devices by JAX's collectives and lax.ppermute only.
A program may use at most 64 MiB of HBM per device.

```python
import math
import jax
import jax.numpy as jnp
import numpy as np
from jax import lax

F = 256
R = 4
NODE_DEV = 16384
POS_DEV = 128
BLOCK = 128
NEG = 32
FAN1 = 4
FAN2 = 2
BLOCKS_DEV = 1
SEED_DEV = 288
H1_DEV = 1152
H2_DEV = 2304
CAP_S = 18
CAP_1 = 72
CAP_2 = 144
NODES = 524288
EDGES = 4096
SEEDS = 9216
H1 = 36864
H2 = 73728
N_DOM = 32


def draw_features(key, part):
    first_key = jax.random.fold_in(key, 0)
    values = jax.random.normal(first_key, (NODES, F), jnp.float32)
    values = jnp.clip(values, -6.0, 6.0)
    return values.astype(jnp.bfloat16)


def place_ends(array, rng, low, high):
    longest = array.shape.index(max(array.shape))
    spots = []
    for shift in (0, 1):
        where = [jax.random.randint(jax.random.fold_in(rng, axis), (), 0, length) for axis, length in enumerate(array.shape)]
        where[longest] = (where[longest] + shift) % array.shape[longest]
        spots.append(tuple(where))
    return array.at[spots[0]].set(low).at[spots[1]].set(high)


def shared_out(rng, own, number, rows, number_of, top, bound, skew):
    sequence = jax.random.permutation(rng, number_of)
    heavy_load, common = portions_of(number_of, rows * top, bound, skew, True), portions_of(number_of, rows * top, bound, skew, False)
    places = jnp.arange(number_of)

    def named(sizes, turn):
        used = int((sizes > 0).sum())
        fixed = max(1, used // 4)
        shifted = fixed + (places - fixed + turn * (used - fixed)) % max(1, number_of - fixed)
        return jnp.zeros((number_of,), jnp.int32).at[sequence[jnp.where(places < fixed, places, shifted)]].set(jnp.asarray(sizes, jnp.int32))

    sizes = jnp.where(number % 4 == 0, named(heavy_load, number // 4), named(common, number - number // 4 - 1))
    mixed = jax.random.permutation(jax.random.fold_in(own, 3), number_of)
    donor, taker = mixed[0:number_of // 2 * 2:2], mixed[1:number_of // 2 * 2:2]
    slack = jnp.minimum(sizes[donor] - 1, bound - sizes[taker]) // 2
    slack = jnp.where((donor == sequence[0]) | (taker == sequence[0]) | (sizes[taker] == 0), 0, jnp.maximum(slack, 0))
    shifted = jax.random.randint(jax.random.fold_in(own, 4), (number_of // 2,), 0, 1 << 20) % (slack + 1)
    sizes = sizes.at[donor].add(-shifted).at[taker].add(shifted)
    members = jnp.searchsorted(jnp.cumsum(sizes), jnp.arange(rows * top), side="right").astype(jnp.int32)
    grid = members.reshape(top, rows).T
    grid = grid[jax.random.permutation(jax.random.fold_in(own, 1), rows)]
    turn = jax.random.randint(jax.random.fold_in(own, 2), (rows, 1), 0, top)
    return jnp.take_along_axis(grid, (jnp.arange(top)[None, :] + turn) % top, axis=1)


def portions_of(amount, total, reach, lean, full):
    loads = [(1 << 20) // math.isqrt(standing ** lean) + 1 for standing in range(1, amount + 1)]
    largest = reach if full else min(reach, max(-(-total // amount), total * loads[0] // sum(loads)))
    least = 1 if total - largest >= amount - 1 else 0
    given, spare = [largest] + [least] * (amount - 1), total - largest - least * (amount - 1)
    while spare > 0:
        movable = [i for i in range(1, amount) if given[i] < largest] or [i for i in range(1, amount) if given[i] < reach]
        mass, remaining = sum([loads[i] for i in movable]), spare
        for i in movable:
            more = min(reach - given[i], max(1, remaining * loads[i] // mass), spare)
            given[i] = given[i] + more
            spare = spare - more
    return np.array(given)


def noise(rng, extent, scale, most, held_as=jnp.bfloat16):
    return jnp.clip(scale * jax.random.normal(rng, extent, jnp.float32), -most, most).astype(held_as)


def setup_inputs(seed: int = 0) -> dict:
    splits = jax.random.split(jax.random.key(seed), 13)
    features = draw_features(jax.random.fold_in(splits[12], 71), 0)
    w_first = noise(splits[1], ((R + 1) * F, F), ((R + 1) * F) ** -0.5, 0.15625)
    w_second = noise(splits[2], ((R + 1) * F, F), ((R + 1) * F) ** -0.5, 0.15625)
    seed_owner_keys = jax.random.split(jax.random.fold_in(splits[3], 1), SEEDS // SEED_DEV)
    seed_owner_turns = jax.random.permutation(jax.random.fold_in(splits[3], 3), SEEDS // SEED_DEV)
    seed_owner = jax.vmap(lambda own, number: shared_out(jax.random.fold_in(splits[3], 2), own, number, SEED_DEV, N_DOM, 1, CAP_S, 2))(seed_owner_keys, seed_owner_turns).reshape((SEEDS, 1))
    seed_row = place_ends(jax.random.randint(splits[4], (SEEDS,), 0, NODE_DEV), jax.random.fold_in(splits[4], 1), 0, NODE_DEV - 1).astype(jnp.int32)
    hop1_owner_keys = jax.random.split(jax.random.fold_in(splits[5], 1), H1 // H1_DEV)
    hop1_owner_turns = jax.random.permutation(jax.random.fold_in(splits[5], 3), H1 // H1_DEV)
    hop1_owner = jax.vmap(lambda own, number: shared_out(jax.random.fold_in(splits[5], 2), own, number, H1_DEV, N_DOM, 1, CAP_1, 2))(hop1_owner_keys, hop1_owner_turns).reshape((H1, 1))
    hop1_row = place_ends(jax.random.randint(splits[6], (H1,), 0, NODE_DEV), jax.random.fold_in(splits[6], 1), 0, NODE_DEV - 1).astype(jnp.int32)
    hop1_rel = place_ends(jax.random.randint(splits[7], (H1,), 0, R), jax.random.fold_in(splits[7], 1), 0, R - 1).astype(jnp.int32)
    hop2_owner_keys = jax.random.split(jax.random.fold_in(splits[8], 1), H2 // H2_DEV)
    hop2_owner_turns = jax.random.permutation(jax.random.fold_in(splits[8], 3), H2 // H2_DEV)
    hop2_owner = jax.vmap(lambda own, number: shared_out(jax.random.fold_in(splits[8], 2), own, number, H2_DEV, N_DOM, 1, CAP_2, 2))(hop2_owner_keys, hop2_owner_turns).reshape((H2, 1))
    hop2_row = place_ends(jax.random.randint(splits[9], (H2,), 0, NODE_DEV), jax.random.fold_in(splits[9], 1), 0, NODE_DEV - 1).astype(jnp.int32)
    hop2_rel = place_ends(jax.random.randint(splits[10], (H2,), 0, R), jax.random.fold_in(splits[10], 1), 0, R - 1).astype(jnp.int32)
    edge_mask = place_ends((jax.random.randint(splits[11], (EDGES,), 0, 4) < 3).astype(jnp.int32), jax.random.fold_in(splits[11], 1), 0, 1)
    return dict(features=features, w_first=w_first, w_second=w_second, seed_owner=seed_owner, seed_row=seed_row, hop1_owner=hop1_owner, hop1_row=hop1_row, hop1_rel=hop1_rel, hop2_owner=hop2_owner, hop2_row=hop2_row, hop2_rel=hop2_rel, edge_mask=edge_mask)


def rgcn_layer(self_rows, neighbours, relations, weights):
    onehot = (relations[..., None] == jnp.arange(R, dtype=jnp.int32)).astype(jnp.float32)
    tallies = jnp.maximum(jnp.sum(onehot, axis=1), 1.0)
    shares = onehot / tallies[:, None, :]
    merged = jnp.einsum('nkr,nkf->nrf', shares, neighbours.astype(jnp.float32)).astype(jnp.bfloat16)
    inputs = jnp.concatenate([self_rows, merged.reshape(self_rows.shape[0], R * F)], axis=1)
    return jnp.dot(inputs, weights, preferred_element_type=jnp.float32)


def edge_scores(second):
    sources = second[:POS_DEV]
    targets = second[POS_DEV:2 * POS_DEV]
    negatives = second[2 * POS_DEV:].reshape(BLOCKS_DEV, NEG, F)
    positive = jnp.sum(sources * targets, axis=1)
    negative = jnp.einsum('bef,bqf->beq', sources.reshape(BLOCKS_DEV, BLOCK, F), negatives,
                          precision=lax.Precision.HIGHEST).reshape(POS_DEV, NEG)
    scores = jnp.concatenate([positive[:, None], negative], axis=1)
    top_score = jnp.max(scores, axis=1, keepdims=True)
    return top_score[:, 0] + jnp.log(jnp.sum(jnp.exp(scores - top_score), axis=1)) - positive


def reference(features, w_first, w_second, seed_owner, seed_row, hop1_owner, hop1_row, hop1_rel,
              hop2_owner, hop2_row, hop2_rel, edge_mask):
    def one_device(pieces):
        s_owner, s_row, a_owner, a_row, a_rel, b_owner, b_row, b_rel = pieces
        x_seed = features[(s_owner * NODE_DEV + s_row).astype(jnp.int32)]
        x_hop1 = features[(a_owner * NODE_DEV + a_row).astype(jnp.int32)]
        x_hop2 = features[(b_owner * NODE_DEV + b_row).astype(jnp.int32)]
        first_hop = jax.nn.relu(rgcn_layer(x_hop1, x_hop2.reshape(H1_DEV, FAN2, F),
                                           b_rel.reshape(H1_DEV, FAN2), w_first)).astype(jnp.bfloat16)
        first_seed = jax.nn.relu(rgcn_layer(x_seed, x_hop1.reshape(SEED_DEV, FAN1, F),
                                            a_rel.reshape(SEED_DEV, FAN1), w_first)).astype(jnp.bfloat16)
        second = rgcn_layer(first_seed, first_hop.reshape(SEED_DEV, FAN1, F),
                            a_rel.reshape(SEED_DEV, FAN1), w_second)
        return edge_scores(second)

    pieces = (seed_owner.reshape(N_DOM, SEED_DEV), seed_row.reshape(N_DOM, SEED_DEV),
              hop1_owner.reshape(N_DOM, H1_DEV), hop1_row.reshape(N_DOM, H1_DEV),
              hop1_rel.reshape(N_DOM, H1_DEV), hop2_owner.reshape(N_DOM, H2_DEV),
              hop2_row.reshape(N_DOM, H2_DEV), hop2_rel.reshape(N_DOM, H2_DEV))
    edge_loss = lax.map(one_device, pieces).reshape(EDGES)
    weights = edge_mask.astype(jnp.float32)
    mean_loss = jnp.sum(weights * edge_loss) / jnp.maximum(jnp.sum(weights), 1.0)
    return edge_loss, mean_loss
```

```python
import functools

import jax
import jax.numpy as jnp
from jax import lax
from jax.experimental import pallas as pl
from jax.experimental.pallas import tpu as pltpu
from jax.sharding import PartitionSpec as P

R = 4
BLOCK = 128
NEG = 32
FAN1 = 4
FAN2 = 2
LANES = 128
F32 = jnp.float32
BF16 = jnp.bfloat16
HIGHEST = lax.Precision.HIGHEST


def round_up(value, unit):
    return (value + unit - 1) // unit * unit


def full(memory_space=pltpu.VMEM):
    return pl.BlockSpec(memory_space=memory_space)


def bucket_kernel(offsets, stride, counts, *refs):
    kinds = len(counts)
    owner_refs, row_refs = refs[:kinds], refs[kinds : 2 * kinds]
    request_ref, slot_ref = refs[2 * kinds :]
    devices, _, width = request_ref.shape
    device = lax.broadcasted_iota(jnp.int32, (devices, LANES), 0)
    before = lax.broadcasted_iota(jnp.int32, (LANES, 2 * LANES), 0)
    lane = lax.broadcasted_iota(jnp.int32, (LANES, 2 * LANES), 1)
    earlier = jnp.where(before < lane, 1.0, 0.0).astype(BF16)
    place = lax.broadcasted_iota(jnp.int32, (width, LANES), 0)
    total = jnp.zeros((2 * devices, width), F32)
    block = 0
    for kind, count in enumerate(counts):
        carried = jnp.zeros((devices, LANES), F32)
        for start in range(0, count, LANES):
            size = min(LANES, count - start)
            owner = owner_refs[kind][:, start : start + size]
            row = row_refs[kind][:, start : start + size]
            if size < LANES:
                owner = jnp.concatenate([owner, jnp.full((1, LANES - size), -1, jnp.int32)], axis=1)
                row = jnp.concatenate([row, jnp.zeros((1, LANES - size), jnp.int32)], axis=1)
            hot = jnp.where(device == owner, 1.0, 0.0)
            ranks = jnp.dot(hot.astype(BF16), earlier, preferred_element_type=F32)
            prior = ranks[:, :LANES] + carried
            carried = carried + ranks[:, LANES:]
            position = jnp.sum(hot * prior, axis=0, keepdims=True).astype(jnp.int32) + offsets[kind]
            slot_ref[block : block + 1, :] = jnp.maximum(owner, 0) * stride + 2 * position
            high = (row // LANES).astype(F32)
            low = (row % LANES).astype(F32)
            halves = jnp.concatenate([hot * high, hot * low], axis=0).astype(BF16)
            spread = jnp.where(place == position, 1.0, 0.0).astype(BF16)
            total = total + lax.dot_general(
                halves, spread, (((1,), (1,)), ((), ())), preferred_element_type=F32
            )
            block += 1
    request = (total[:devices] * (2.0 * LANES) + total[devices:] * 2.0).astype(jnp.int32)
    request_ref[...] = request.reshape(devices, 1, width)


def gather_kernel(slots, chunk, request_ref, table_ref, out_ref, staged, wide, packed, sems):
    devices = out_ref.shape[0]
    rows = table_ref.shape[0]
    pieces = rows // chunk

    def copy(piece):
        span = pl.ds(piece * chunk, chunk)
        return pltpu.make_async_copy(table_ref.at[span], staged.at[span], sems.at[piece])

    for piece in range(pieces):
        copy(piece).start()
    step = min(chunk, 256)
    for piece in range(pieces):
        copy(piece).wait()

        def widen(index, _):
            base = pl.multiple_of(piece * chunk + index * step, step)
            values = staged[pl.ds(base, step), :].astype(F32)
            wide[pl.ds(2 * base, step, stride=2), :] = values[:, :LANES]
            wide[pl.ds(2 * base + 1, step, stride=2), :] = values[:, LANES:]
            return 0

        lax.fori_loop(0, chunk // step, widen, 0)

    def serve(device, _):
        for slot in range(slots):
            row = pl.multiple_of(request_ref[device, 0, slot], 2)
            packed[pl.ds(2 * slot, 2), :] = wide[pl.ds(row, 2), :]
        out_ref[device] = packed[: 2 * slots, :].astype(BF16)
        return 0

    lax.fori_loop(0, devices, serve, 0)


def layer(selves, neighbours, share, weights):
    pieces = list(selves)
    fan = len(neighbours)
    for relation in range(R):
        for half in range(2):
            merged = share(relation, 0) * neighbours[0][half]
            for k in range(1, fan):
                merged = merged + share(relation, k) * neighbours[k][half]
            pieces.append(merged)
    inputs = jnp.concatenate([piece.astype(BF16) for piece in pieces], axis=1)
    return jnp.dot(inputs, weights, preferred_element_type=F32)


def model_kernel(
    counts, stride, slot_ref, got_ref, first_ref, second_ref, share1_ref, share2_ref, mask_ref,
    loss_ref, sums_ref, wide, x0, x1, x2, h_low, h_high,
):
    devices, held, _ = got_ref.shape
    seeds, firsts, _ = counts

    def widen(device, _):
        wide[pl.ds(pl.multiple_of(device * stride, 8), held), :] = got_ref[device].astype(F32)
        return 0

    lax.fori_loop(0, devices, widen, 0)
    block = 0
    for target, count in zip((x0, x1, x2), counts):
        whole = count // LANES

        def fetch(index, _, target=target, block=block):
            base = pl.multiple_of(index * 2 * LANES, 2 * LANES)
            for lane in range(LANES):
                slot = pl.multiple_of(slot_ref[block + index, lane], 2)
                target[pl.ds(base + 2 * lane, 2), :] = wide[pl.ds(slot, 2), :]
            return 0

        lax.fori_loop(0, whole, fetch, 0)
        for lane in range(count - whole * LANES):
            slot = pl.multiple_of(slot_ref[block + whole, lane], 2)
            target[pl.ds(2 * (whole * LANES + lane), 2), :] = wide[pl.ds(slot, 2), :]
        block += -(-count // LANES)

    step = LANES

    def hop(index, _):
        base = pl.multiple_of(index * step, step)
        selves = [x1[pl.ds(2 * base + half, step, stride=2), :] for half in range(2)]
        neighbours = [
            [x2[pl.ds(2 * FAN2 * base + 2 * k + half, step, stride=2 * FAN2), :] for half in range(2)]
            for k in range(FAN2)
        ]
        shares = share2_ref[pl.ds(base, step), :]
        hidden = layer(
            selves, neighbours, lambda r, k: shares[:, r * FAN2 + k : r * FAN2 + k + 1], first_ref[...]
        )
        hidden = jnp.maximum(hidden, 0.0).astype(BF16).astype(F32)
        h_low[pl.ds(base, step), :] = hidden[:, :LANES]
        h_high[pl.ds(base, step), :] = hidden[:, LANES:]
        return 0

    lax.fori_loop(0, firsts // step, hop, 0)
    shares = share1_ref[...]
    share = lambda r, k: shares[:, r * FAN1 + k : r * FAN1 + k + 1]
    selves = [x0[pl.ds(half, seeds, stride=2), :] for half in range(2)]
    neighbours = [
        [x1[pl.ds(2 * k + half, seeds, stride=2 * FAN1), :] for half in range(2)] for k in range(FAN1)
    ]
    hidden = jnp.maximum(layer(selves, neighbours, share, first_ref[...]), 0.0).astype(BF16)
    selves = [hidden[:, :LANES], hidden[:, LANES:]]
    neighbours = [
        [h[pl.ds(k, seeds, stride=FAN1), :] for h in (h_low, h_high)] for k in range(FAN1)
    ]
    second = layer(selves, neighbours, share, second_ref[...])
    positives = mask_ref.shape[1]
    width = second.shape[1]
    contract = (((1,), (1,)), ((), ()))
    loss_sum = jnp.zeros((1, 1), F32)
    for number in range(positives // BLOCK):
        span = slice(number * BLOCK, (number + 1) * BLOCK)
        sources = second[span]
        targets = second[positives + number * BLOCK : positives + (number + 1) * BLOCK]
        negatives = second[2 * positives + number * NEG : 2 * positives + (number + 1) * NEG]
        positive = lax.dot_general(
            jnp.ones((8, width), F32), sources * targets, contract, precision=HIGHEST,
            preferred_element_type=F32,
        )[:1]
        negative = lax.dot_general(
            negatives, sources, contract, precision=HIGHEST, preferred_element_type=F32
        )
        top = jnp.maximum(jnp.max(negative, axis=0, keepdims=True), positive)
        spread = jnp.sum(jnp.exp(negative - top), axis=0, keepdims=True) + jnp.exp(positive - top)
        loss = top + jnp.log(spread) - positive
        loss_ref[:, span] = loss
        loss_sum = loss_sum + jnp.sum(
            mask_ref[:, span].astype(F32) * loss, axis=1, keepdims=True
        )
    edge_sum = jnp.sum(mask_ref[...].astype(F32), axis=1, keepdims=True)
    lane = lax.broadcasted_iota(jnp.int32, (devices, 1, LANES), 2)
    sums_ref[...] = jnp.where(
        lane == 0, loss_sum.reshape(1, 1, 1), jnp.where(lane == 1, edge_sum.reshape(1, 1, 1), 0.0)
    )


def mean_shares(relations):
    onehot = (relations[..., None] == jnp.arange(R, dtype=jnp.int32)).astype(F32)
    tallies = jnp.maximum(jnp.sum(onehot, axis=1), 1.0)
    shares = onehot / tallies[:, None, :]
    return jnp.transpose(shares, (0, 2, 1)).reshape(relations.shape[0], -1)


def exchange(array):
    return lax.all_to_all(array, "dom", split_axis=0, concat_axis=0, tiled=True)


def shards(
    features, w_first, w_second, seed_owner, seed_row, hop1_owner, hop1_row, hop1_rel,
    hop2_owner, hop2_row, hop2_rel, edge_mask,
):
    devices = lax.axis_size("dom")
    nodes, width = features.shape
    owners = (seed_owner, hop1_owner, hop2_owner)
    rows = (seed_row, hop1_row, hop2_row)
    counts = tuple(row.shape[0] for row in rows)
    capacities = [(2 * count + devices - 1) // devices for count in counts]
    offsets = [sum(capacities[:kind]) for kind in range(len(counts))]
    slots = sum(capacities)
    held = 2 * slots
    stride = round_up(held, 8)
    blocks = sum(-(-count // LANES) for count in counts)

    requests, places = pl.pallas_call(
        functools.partial(bucket_kernel, offsets, stride, counts),
        out_shape=(
            jax.ShapeDtypeStruct((devices, 1, round_up(slots, LANES)), jnp.int32),
            jax.ShapeDtypeStruct((blocks, LANES), jnp.int32),
        ),
        in_specs=[full()] * 6,
        out_specs=(full(), full()),
        name="bucket",
    )(*[owner.reshape(1, -1) for owner in owners], *[row.reshape(1, -1) for row in rows])

    arrived = exchange(requests)
    chunk = nodes // 16
    located = pl.pallas_call(
        functools.partial(gather_kernel, slots, chunk),
        out_shape=jax.ShapeDtypeStruct((devices, held, LANES), BF16),
        in_specs=[full(pltpu.SMEM), full(pl.ANY)],
        out_specs=full(),
        scratch_shapes=[
            pltpu.VMEM((nodes, width), BF16),
            pltpu.VMEM((2 * nodes, LANES), F32),
            pltpu.VMEM((stride, LANES), F32),
            pltpu.SemaphoreType.DMA((nodes // chunk,)),
        ],
        name="owner_gather",
    )(arrived, features)
    returned = exchange(located)

    share1 = mean_shares(hop1_rel.reshape(counts[0], FAN1))
    share2 = mean_shares(hop2_rel.reshape(counts[1], FAN2))
    positives = edge_mask.shape[0]
    loss, sums = pl.pallas_call(
        functools.partial(model_kernel, counts, stride),
        out_shape=(
            jax.ShapeDtypeStruct((1, positives), F32),
            jax.ShapeDtypeStruct((devices, 1, LANES), F32),
        ),
        in_specs=[full(pltpu.SMEM)] + [full()] * 6,
        out_specs=(full(), full()),
        scratch_shapes=[pltpu.VMEM((devices * stride, LANES), F32)]
        + [pltpu.VMEM((2 * count, LANES), F32) for count in counts]
        + [pltpu.VMEM((counts[1], LANES), F32)] * 2,
        name="model",
    )(places, returned, w_first, w_second, share1, share2, edge_mask.reshape(1, -1))
    totals = jnp.sum(exchange(sums), axis=(0, 1))
    mean_loss = totals[0] / jnp.maximum(totals[1], 1.0)
    return (loss.reshape(positives), mean_loss)


def solution(mesh):
    placed = (
        P("dom", None), P(), P(), P("dom", None), P("dom"), P("dom", None), P("dom"), P("dom"),
        P("dom", None), P("dom"), P("dom"), P("dom"),
    )
    return jax.shard_map(
        shards, mesh=mesh, in_specs=placed, out_specs=(P("dom"), P()), check_vma=False
    )
```

```python
import functools

import jax
import jax.numpy as jnp
from jax import lax
from jax.experimental import pallas as pl
from jax.experimental.pallas import tpu as pltpu
from jax.sharding import PartitionSpec as P

R = 4
BLOCK = 128
NEG = 32
FAN1 = 4
FAN2 = 2
LANES = 128
F32 = jnp.float32
BF16 = jnp.bfloat16
HIGHEST = lax.Precision.HIGHEST


def round_up(value, unit):
    return (value + unit - 1) // unit * unit


def full(memory_space=pltpu.VMEM):
    return pl.BlockSpec(memory_space=memory_space)


def bucket_kernel(offsets, starts, strides, counts, *refs):
    kinds = len(counts)
    owner_refs, row_refs = refs[:kinds], refs[kinds : 2 * kinds]
    request_ref, slot_ref = refs[2 * kinds :]
    devices, _, width = request_ref.shape
    device = lax.broadcasted_iota(jnp.int32, (devices, LANES), 0)
    before = lax.broadcasted_iota(jnp.int32, (LANES, 2 * LANES), 0)
    lane = lax.broadcasted_iota(jnp.int32, (LANES, 2 * LANES), 1)
    earlier = jnp.where(before < lane, 1.0, 0.0).astype(BF16)
    place = lax.broadcasted_iota(jnp.int32, (width, LANES), 0)
    total = jnp.zeros((2 * devices, width), F32)
    block = 0
    for kind, count in enumerate(counts):
        carried = jnp.zeros((devices, LANES), F32)
        for start in range(0, count, LANES):
            size = min(LANES, count - start)
            owner = owner_refs[kind][:, start : start + size]
            row = row_refs[kind][:, start : start + size]
            if size < LANES:
                owner = jnp.concatenate([owner, jnp.full((1, LANES - size), -1, jnp.int32)], axis=1)
                row = jnp.concatenate([row, jnp.zeros((1, LANES - size), jnp.int32)], axis=1)
            hot = jnp.where(device == owner, 1.0, 0.0)
            ranks = jnp.dot(hot.astype(BF16), earlier, preferred_element_type=F32)
            prior = ranks[:, :LANES] + carried
            carried = carried + ranks[:, LANES:]
            position = jnp.sum(hot * prior, axis=0, keepdims=True).astype(jnp.int32) + offsets[kind]
            slot_ref[block : block + 1, :] = (
                jnp.maximum(owner, 0) * strides[kind] + 2 * (position - starts[kind])
            )
            high = (row // LANES).astype(F32)
            low = (row % LANES).astype(F32)
            halves = jnp.concatenate([hot * high, hot * low], axis=0).astype(BF16)
            spread = jnp.where(place == position, 1.0, 0.0).astype(BF16)
            total = total + lax.dot_general(
                halves, spread, (((1,), (1,)), ((), ())), preferred_element_type=F32
            )
            block += 1
    request = (total[:devices] * (2.0 * LANES) + total[devices:] * 2.0).astype(jnp.int32)
    request_ref[...] = request.reshape(devices, 1, width)


def gather_kernel(first, slots, chunk, request_ref, table_ref, out_ref, staged, wide, packed, sems):
    devices = out_ref.shape[0]
    rows = table_ref.shape[0]
    pieces = rows // chunk

    def copy(piece):
        span = pl.ds(piece * chunk, chunk)
        return pltpu.make_async_copy(table_ref.at[span], staged.at[span], sems.at[piece])

    for piece in range(pieces):
        copy(piece).start()
    step = min(chunk, 256)
    for piece in range(pieces):
        copy(piece).wait()

        def widen(index, _):
            base = pl.multiple_of(piece * chunk + index * step, step)
            values = staged[pl.ds(base, step), :].astype(F32)
            wide[pl.ds(2 * base, step, stride=2), :] = values[:, :LANES]
            wide[pl.ds(2 * base + 1, step, stride=2), :] = values[:, LANES:]
            return 0

        lax.fori_loop(0, chunk // step, widen, 0)

    def serve(device, _):
        for slot in range(slots):
            row = pl.multiple_of(request_ref[device, 0, first + slot], 2)
            packed[pl.ds(2 * slot, 2), :] = wide[pl.ds(row, 2), :]
        out_ref[device] = packed[: 2 * slots, :].astype(BF16)
        return 0

    lax.fori_loop(0, devices, serve, 0)


def layer(selves, neighbours, share, weights):
    pieces = list(selves)
    fan = len(neighbours)
    for relation in range(R):
        for half in range(2):
            merged = share(relation, 0) * neighbours[0][half]
            for k in range(1, fan):
                merged = merged + share(relation, k) * neighbours[k][half]
            pieces.append(merged)
    inputs = jnp.concatenate([piece.astype(BF16) for piece in pieces], axis=1)
    return jnp.dot(inputs, weights, preferred_element_type=F32)


def widen_rows(got_ref, wide, stride):
    devices, held, _ = got_ref.shape

    def widen(device, _):
        wide[pl.ds(pl.multiple_of(device * stride, 8), held), :] = got_ref[device].astype(F32)
        return 0

    lax.fori_loop(0, devices, widen, 0)


def fetch_rows(slot_ref, block, wide, target, count):
    whole = count // LANES

    def fetch(index, _):
        base = pl.multiple_of(index * 2 * LANES, 2 * LANES)
        for lane in range(LANES):
            slot = pl.multiple_of(slot_ref[block + index, lane], 2)
            target[pl.ds(base + 2 * lane, 2), :] = wide[pl.ds(slot, 2), :]
        return 0

    lax.fori_loop(0, whole, fetch, 0)
    for lane in range(count - whole * LANES):
        slot = pl.multiple_of(slot_ref[block + whole, lane], 2)
        target[pl.ds(2 * (whole * LANES + lane), 2), :] = wide[pl.ds(slot, 2), :]
    return block + -(-count // LANES)


def early_kernel(
    seeds, firsts, stride, slot_ref, got_ref, first_ref, share1_ref, hidden_ref, base_ref,
    wide, x0, x1,
):
    widen_rows(got_ref, wide, stride)
    block = fetch_rows(slot_ref, 0, wide, x0, seeds)
    fetch_rows(slot_ref, block, wide, x1, firsts)
    step = LANES
    width = first_ref.shape[1]

    def hop(index, _):
        base = pl.multiple_of(index * step, step)
        selves = [x1[pl.ds(2 * base + half, step, stride=2), :] for half in range(2)]
        inputs = jnp.concatenate([piece.astype(BF16) for piece in selves], axis=1)
        base_ref[pl.ds(base, step), :] = jnp.dot(
            inputs, first_ref[:width, :], preferred_element_type=F32
        )
        return 0

    lax.fori_loop(0, firsts // step, hop, 0)
    shares = share1_ref[...]
    share = lambda r, k: shares[:, r * FAN1 + k : r * FAN1 + k + 1]
    selves = [x0[pl.ds(half, seeds, stride=2), :] for half in range(2)]
    neighbours = [
        [x1[pl.ds(2 * k + half, seeds, stride=2 * FAN1), :] for half in range(2)] for k in range(FAN1)
    ]
    hidden = layer(selves, neighbours, share, first_ref[...])
    hidden_ref[...] = jnp.maximum(hidden, 0.0).astype(BF16)


def late_kernel(
    block, counts, stride, slot_ref, got_ref, base_ref, hidden_ref, first_ref, second_ref,
    share1_ref, share2_ref, mask_ref, loss_ref, sums_ref, wide, x2, h_low, h_high,
):
    devices = got_ref.shape[0]
    seeds, firsts, seconds = counts
    width = first_ref.shape[1]
    widen_rows(got_ref, wide, stride)
    fetch_rows(slot_ref, block, wide, x2, seconds)
    step = LANES

    def hop(index, _):
        base = pl.multiple_of(index * step, step)
        neighbours = [
            [x2[pl.ds(2 * FAN2 * base + 2 * k + half, step, stride=2 * FAN2), :] for half in range(2)]
            for k in range(FAN2)
        ]
        shares = share2_ref[pl.ds(base, step), :]
        hidden = base_ref[pl.ds(base, step), :] + layer(
            [], neighbours, lambda r, k: shares[:, r * FAN2 + k : r * FAN2 + k + 1],
            first_ref[width:, :],
        )
        hidden = jnp.maximum(hidden, 0.0).astype(BF16).astype(F32)
        h_low[pl.ds(base, step), :] = hidden[:, :LANES]
        h_high[pl.ds(base, step), :] = hidden[:, LANES:]
        return 0

    lax.fori_loop(0, firsts // step, hop, 0)
    shares = share1_ref[...]
    share = lambda r, k: shares[:, r * FAN1 + k : r * FAN1 + k + 1]
    hidden = hidden_ref[...]
    selves = [hidden[:, :LANES], hidden[:, LANES:]]
    neighbours = [
        [h[pl.ds(k, seeds, stride=FAN1), :] for h in (h_low, h_high)] for k in range(FAN1)
    ]
    second = layer(selves, neighbours, share, second_ref[...])
    positives = mask_ref.shape[1]
    contract = (((1,), (1,)), ((), ()))
    loss_sum = jnp.zeros((1, 1), F32)
    for number in range(positives // BLOCK):
        span = slice(number * BLOCK, (number + 1) * BLOCK)
        sources = second[span]
        targets = second[positives + number * BLOCK : positives + (number + 1) * BLOCK]
        negatives = second[2 * positives + number * NEG : 2 * positives + (number + 1) * NEG]
        positive = lax.dot_general(
            jnp.ones((8, width), F32), sources * targets, contract, precision=HIGHEST,
            preferred_element_type=F32,
        )[:1]
        negative = lax.dot_general(
            negatives, sources, contract, precision=HIGHEST, preferred_element_type=F32
        )
        top = jnp.maximum(jnp.max(negative, axis=0, keepdims=True), positive)
        spread = jnp.sum(jnp.exp(negative - top), axis=0, keepdims=True) + jnp.exp(positive - top)
        loss = top + jnp.log(spread) - positive
        loss_ref[:, span] = loss
        loss_sum = loss_sum + jnp.sum(
            mask_ref[:, span].astype(F32) * loss, axis=1, keepdims=True
        )
    edge_sum = jnp.sum(mask_ref[...].astype(F32), axis=1, keepdims=True)
    lane = lax.broadcasted_iota(jnp.int32, (devices, 1, LANES), 2)
    sums_ref[...] = jnp.where(
        lane == 0, loss_sum.reshape(1, 1, 1), jnp.where(lane == 1, edge_sum.reshape(1, 1, 1), 0.0)
    )


def mean_shares(relations):
    onehot = (relations[..., None] == jnp.arange(R, dtype=jnp.int32)).astype(F32)
    tallies = jnp.maximum(jnp.sum(onehot, axis=1), 1.0)
    shares = onehot / tallies[:, None, :]
    return jnp.transpose(shares, (0, 2, 1)).reshape(relations.shape[0], -1)


def exchange(array):
    return lax.all_to_all(array, "dom", split_axis=0, concat_axis=0, tiled=True)


def shards(
    features, w_first, w_second, seed_owner, seed_row, hop1_owner, hop1_row, hop1_rel,
    hop2_owner, hop2_row, hop2_rel, edge_mask,
):
    devices = lax.axis_size("dom")
    nodes, width = features.shape
    owners = (seed_owner, hop1_owner, hop2_owner)
    rows = (seed_row, hop1_row, hop2_row)
    counts = tuple(row.shape[0] for row in rows)
    capacities = [(2 * count + devices - 1) // devices for count in counts]
    offsets = [sum(capacities[:kind]) for kind in range(len(counts))]
    slots = sum(capacities)
    groups = ((0, offsets[2]), (offsets[2], slots))
    pitches = [round_up(2 * (end - start), 8) for start, end in groups]
    group_of = (0, 0, 1)
    blocks = [-(-count // LANES) for count in counts]

    requests, places = pl.pallas_call(
        functools.partial(
            bucket_kernel, offsets, [groups[g][0] for g in group_of],
            [pitches[g] for g in group_of], counts,
        ),
        out_shape=(
            jax.ShapeDtypeStruct((devices, 1, round_up(slots, LANES)), jnp.int32),
            jax.ShapeDtypeStruct((sum(blocks), LANES), jnp.int32),
        ),
        in_specs=[full()] * 6,
        out_specs=(full(), full()),
        name="bucket",
    )(*[owner.reshape(1, -1) for owner in owners], *[row.reshape(1, -1) for row in rows])

    arrived = exchange(requests)
    chunk = nodes // 16

    def locate(start, end):
        held = 2 * (end - start)
        return pl.pallas_call(
            functools.partial(gather_kernel, start, end - start, chunk),
            out_shape=jax.ShapeDtypeStruct((devices, held, LANES), BF16),
            in_specs=[full(pltpu.SMEM), full(pl.ANY)],
            out_specs=full(),
            scratch_shapes=[
                pltpu.VMEM((nodes, width), BF16),
                pltpu.VMEM((2 * nodes, LANES), F32),
                pltpu.VMEM((round_up(held, 8), LANES), F32),
                pltpu.SemaphoreType.DMA((nodes // chunk,)),
            ],
            cost_estimate=pl.CostEstimate(flops=20_000_000, bytes_accessed=nodes * width * 2, transcendentals=0),
            name="owner_gather",
        )(arrived, features)

    share1 = mean_shares(hop1_rel.reshape(counts[0], FAN1))
    share2 = mean_shares(hop2_rel.reshape(counts[1], FAN2))
    located = locate(*groups[0])
    near = exchange(located)
    located = locate(*groups[1])
    far = exchange(located)
    hidden, base = pl.pallas_call(
        functools.partial(early_kernel, counts[0], counts[1], pitches[0]),
        out_shape=(
            jax.ShapeDtypeStruct((counts[0], width), BF16),
            jax.ShapeDtypeStruct((counts[1], width), F32),
        ),
        in_specs=[full(pltpu.SMEM)] + [full()] * 3,
        out_specs=(full(), full()),
        scratch_shapes=[pltpu.VMEM((devices * pitches[0], LANES), F32)]
        + [pltpu.VMEM((2 * count, LANES), F32) for count in counts[:2]],
        name="early",
    )(places, near, w_first, share1)
    positives = edge_mask.shape[0]
    loss, sums = pl.pallas_call(
        functools.partial(late_kernel, blocks[0] + blocks[1], counts, pitches[1]),
        out_shape=(
            jax.ShapeDtypeStruct((1, positives), F32),
            jax.ShapeDtypeStruct((devices, 1, LANES), F32),
        ),
        in_specs=[full(pltpu.SMEM)] + [full()] * 8,
        out_specs=(full(), full()),
        scratch_shapes=[
            pltpu.VMEM((devices * pitches[1], LANES), F32),
            pltpu.VMEM((2 * counts[2], LANES), F32),
        ]
        + [pltpu.VMEM((counts[1], LANES), F32)] * 2,
        name="late",
    )(places, far, base, hidden, w_first, w_second, share1, share2, edge_mask.reshape(1, -1))
    totals = jnp.sum(exchange(sums), axis=(0, 1))
    mean_loss = totals[0] / jnp.maximum(totals[1], 1.0)
    return (loss.reshape(positives), mean_loss)


def solution(mesh):
    placed = (
        P("dom", None), P(), P(), P("dom", None), P("dom"), P("dom", None), P("dom"), P("dom"),
        P("dom", None), P("dom"), P("dom"), P("dom"),
    )
    return jax.shard_map(
        shards, mesh=mesh, in_specs=placed, out_specs=(P("dom"), P()), check_vma=False
    )
```

```python
import functools

import jax
import jax.numpy as jnp
from jax import lax
from jax.experimental import pallas as pl
from jax.experimental.pallas import tpu as pltpu
from jax.sharding import PartitionSpec as P

R = 4
BLOCK = 128
NEG = 32
FAN1 = 4
FAN2 = 2
LANES = 128
PARTS = 4
HOP_STEP = 384
F32 = jnp.float32
BF16 = jnp.bfloat16
HIGHEST = lax.Precision.HIGHEST


def round_up(value, unit):
    return (value + unit - 1) // unit * unit


def full(memory_space=pltpu.VMEM):
    return pl.BlockSpec(memory_space=memory_space)


def bucket_kernel(offsets, stride, counts, *refs):
    kinds = len(counts)
    owner_refs, row_refs = refs[:kinds], refs[kinds : 2 * kinds]
    request_ref, slot_ref = refs[2 * kinds :]
    devices, _, width = request_ref.shape
    device = lax.broadcasted_iota(jnp.int32, (devices, LANES), 0)
    before = lax.broadcasted_iota(jnp.int32, (LANES, 2 * LANES), 0)
    lane = lax.broadcasted_iota(jnp.int32, (LANES, 2 * LANES), 1)
    earlier = jnp.where(before < lane, 1.0, 0.0).astype(BF16)
    place = lax.broadcasted_iota(jnp.int32, (width, LANES), 0)
    total = jnp.zeros((2 * devices, width), F32)
    block = 0
    for kind, count in enumerate(counts):
        carried = jnp.zeros((devices, LANES), F32)
        for start in range(0, count, LANES):
            size = min(LANES, count - start)
            owner = owner_refs[kind][:, start : start + size]
            row = row_refs[kind][pl.ds(start, size)].reshape(1, size)
            if size < LANES:
                owner = jnp.concatenate([owner, jnp.full((1, LANES - size), -1, jnp.int32)], axis=1)
                row = jnp.concatenate([row, jnp.zeros((1, LANES - size), jnp.int32)], axis=1)
            hot = jnp.where(device == owner, 1.0, 0.0)
            ranks = jnp.dot(hot.astype(BF16), earlier, preferred_element_type=F32)
            prior = ranks[:, :LANES] + carried
            carried = carried + ranks[:, LANES:]
            position = jnp.sum(hot * prior, axis=0, keepdims=True).astype(jnp.int32) + offsets[kind]
            slot_ref[block : block + 1, :] = jnp.maximum(owner, 0) * stride + 2 * position
            high = (row // LANES).astype(F32)
            low = (row % LANES).astype(F32)
            halves = jnp.concatenate([hot * high, hot * low], axis=0).astype(BF16)
            spread = jnp.where(place == position, 1.0, 0.0).astype(BF16)
            total = total + lax.dot_general(
                halves, spread, (((1,), (1,)), ((), ())), preferred_element_type=F32
            )
            block += 1
    request = (total[:devices] * (2.0 * LANES) + total[devices:] * 2.0).astype(jnp.int32)
    request_ref[...] = request.reshape(devices, 1, width)


def gather_kernel(
    slots, chunk, group, request_ref, table_ref, out_ref, request, staged, wide, packed, rows_out,
    request_sem, sems, out_sems,
):
    devices = out_ref.shape[0]
    pieces = table_ref.shape[0] // chunk
    asked = pltpu.make_async_copy(request_ref, request, request_sem)
    asked.start()

    def copy(piece):
        span = pl.ds(piece * chunk, chunk)
        return pltpu.make_async_copy(table_ref.at[span], staged.at[span], sems.at[piece])

    for piece in range(pieces):
        copy(piece).start()
    step = min(chunk, 256)
    for piece in range(pieces):
        copy(piece).wait()

        def widen(index, _):
            base = pl.multiple_of(piece * chunk + index * step, step)
            values = staged[pl.ds(base, step), :].astype(F32)
            wide[pl.ds(2 * base, step, stride=2), :] = values[:, :LANES]
            wide[pl.ds(2 * base + 1, step, stride=2), :] = values[:, LANES:]
            return 0

        lax.fori_loop(0, chunk // step, widen, 0)
    asked.wait()

    def serve(device, _):
        for slot in range(slots):
            row = pl.multiple_of(request[device, 0, slot], 2)
            packed[pl.ds(2 * slot, 2), :] = wide[pl.ds(row, 2), :]
        rows_out[device] = packed[: 2 * slots, :].astype(BF16)
        return 0

    def leave(part):
        span = pl.ds(part * group, group)
        return pltpu.make_async_copy(rows_out.at[span], out_ref.at[span], out_sems.at[part])

    for part in range(devices // group):
        lax.fori_loop(part * group, (part + 1) * group, serve, 0)
        leave(part).start()
    for part in range(devices // group):
        leave(part).wait()


def layer(selves, neighbours, share, weights):
    pieces = list(selves)
    fan = len(neighbours)
    for relation in range(R):
        for half in range(2):
            merged = share(relation, 0) * neighbours[0][half]
            for k in range(1, fan):
                merged = merged + share(relation, k) * neighbours[k][half]
            pieces.append(merged)
    inputs = jnp.concatenate([piece.astype(BF16) for piece in pieces], axis=1)
    return jnp.dot(inputs, weights, preferred_element_type=F32)


def model_kernel(
    counts, stride, group, slot_hbm, got_hbm, first_hbm, second_hbm, share1_ref, share2_ref, mask_ref,
    loss_ref, sums_ref, slot_ref, got, first_ref, second_ref, wide, x0, x1, x2, h_low, h_high, sems,
    got_sems,
):
    devices, held, _ = got_hbm.shape
    seeds, firsts, _ = counts

    def arrive(part):
        span = pl.ds(part * group, group)
        return pltpu.make_async_copy(got_hbm.at[span], got.at[span], got_sems.at[part])

    for part in range(devices // group):
        arrive(part).start()
    side = [
        pltpu.make_async_copy(source, target, sems.at[number])
        for number, (source, target) in enumerate(
            ((slot_hbm, slot_ref), (first_hbm, first_ref), (second_hbm, second_ref))
        )
    ]
    for copy in side:
        copy.start()

    def widen(device, _):
        wide[pl.ds(pl.multiple_of(device * stride, 8), held), :] = got[device].astype(F32)
        return 0

    for part in range(devices // group):
        arrive(part).wait()
        lax.fori_loop(part * group, (part + 1) * group, widen, 0)
    side[0].wait()
    block = 0
    for target, count in zip((x0, x1, x2), counts):
        whole = count // LANES

        def fetch(index, _, target=target, block=block):
            base = pl.multiple_of(index * 2 * LANES, 2 * LANES)
            for lane in range(LANES):
                slot = pl.multiple_of(slot_ref[block + index, lane], 2)
                target[pl.ds(base + 2 * lane, 2), :] = wide[pl.ds(slot, 2), :]
            return 0

        lax.fori_loop(0, whole, fetch, 0)
        for lane in range(count - whole * LANES):
            slot = pl.multiple_of(slot_ref[block + whole, lane], 2)
            target[pl.ds(2 * (whole * LANES + lane), 2), :] = wide[pl.ds(slot, 2), :]
        block += -(-count // LANES)

    step = HOP_STEP
    side[1].wait()
    side[2].wait()

    def hop(index, _):
        base = pl.multiple_of(index * step, step)
        selves = [x1[pl.ds(2 * base + half, step, stride=2), :] for half in range(2)]
        neighbours = [
            [x2[pl.ds(2 * FAN2 * base + 2 * k + half, step, stride=2 * FAN2), :] for half in range(2)]
            for k in range(FAN2)
        ]
        shares = share2_ref[pl.ds(base, step), :]
        hidden = layer(
            selves, neighbours, lambda r, k: shares[:, r * FAN2 + k : r * FAN2 + k + 1], first_ref[...]
        )
        hidden = jnp.maximum(hidden, 0.0).astype(BF16).astype(F32)
        h_low[pl.ds(base, step), :] = hidden[:, :LANES]
        h_high[pl.ds(base, step), :] = hidden[:, LANES:]
        return 0

    lax.fori_loop(0, firsts // step, hop, 0)
    shares = share1_ref[...]
    share = lambda r, k: shares[:, r * FAN1 + k : r * FAN1 + k + 1]
    selves = [x0[pl.ds(half, seeds, stride=2), :] for half in range(2)]
    neighbours = [
        [x1[pl.ds(2 * k + half, seeds, stride=2 * FAN1), :] for half in range(2)] for k in range(FAN1)
    ]
    hidden = jnp.maximum(layer(selves, neighbours, share, first_ref[...]), 0.0).astype(BF16)
    selves = [hidden[:, :LANES], hidden[:, LANES:]]
    neighbours = [
        [h[pl.ds(k, seeds, stride=FAN1), :] for h in (h_low, h_high)] for k in range(FAN1)
    ]
    second = layer(selves, neighbours, share, second_ref[...])
    positives = mask_ref.shape[1]
    width = second.shape[1]
    contract = (((1,), (1,)), ((), ()))
    loss_sum = jnp.zeros((1, 1), F32)
    for number in range(positives // BLOCK):
        span = slice(number * BLOCK, (number + 1) * BLOCK)
        sources = second[span]
        targets = second[positives + number * BLOCK : positives + (number + 1) * BLOCK]
        negatives = second[2 * positives + number * NEG : 2 * positives + (number + 1) * NEG]
        positive = lax.dot_general(
            jnp.ones((8, width), F32), sources * targets, contract, precision=HIGHEST,
            preferred_element_type=F32,
        )[:1]
        negative = lax.dot_general(
            negatives, sources, contract, precision=HIGHEST, preferred_element_type=F32
        )
        top = jnp.maximum(jnp.max(negative, axis=0, keepdims=True), positive)
        spread = jnp.sum(jnp.exp(negative - top), axis=0, keepdims=True) + jnp.exp(positive - top)
        loss = top + jnp.log(spread) - positive
        loss_ref[:, span] = loss
        loss_sum = loss_sum + jnp.sum(
            mask_ref[:, span].astype(F32) * loss, axis=1, keepdims=True
        )
    edge_sum = jnp.sum(mask_ref[...].astype(F32), axis=1, keepdims=True)
    lane = lax.broadcasted_iota(jnp.int32, (devices, 1, LANES), 2)
    sums_ref[...] = jnp.where(
        lane == 0, loss_sum.reshape(1, 1, 1), jnp.where(lane == 1, edge_sum.reshape(1, 1, 1), 0.0)
    )


def mean_shares(relations):
    onehot = (relations[..., None] == jnp.arange(R, dtype=jnp.int32)).astype(F32)
    tallies = jnp.maximum(jnp.sum(onehot, axis=1), 1.0)
    shares = onehot / tallies[:, None, :]
    return jnp.transpose(shares, (0, 2, 1)).reshape(relations.shape[0], -1)


def exchange(array):
    return lax.all_to_all(array, "dom", split_axis=0, concat_axis=0, tiled=True)


def shards(
    features, w_first, w_second, seed_owner, seed_row, hop1_owner, hop1_row, hop1_rel,
    hop2_owner, hop2_row, hop2_rel, edge_mask,
):
    devices = lax.axis_size("dom")
    nodes, width = features.shape
    owners = (seed_owner, hop1_owner, hop2_owner)
    rows = (seed_row, hop1_row, hop2_row)
    counts = tuple(row.shape[0] for row in rows)
    capacities = [(2 * count + devices - 1) // devices for count in counts]
    offsets = [sum(capacities[:kind]) for kind in range(len(counts))]
    slots = sum(capacities)
    held = 2 * slots
    stride = round_up(held, 8)
    blocks = sum(-(-count // LANES) for count in counts)

    requests, places = pl.pallas_call(
        functools.partial(bucket_kernel, offsets, stride, counts),
        out_shape=(
            jax.ShapeDtypeStruct((devices, 1, round_up(slots, LANES)), jnp.int32),
            jax.ShapeDtypeStruct((blocks, LANES), jnp.int32),
        ),
        in_specs=[full()] * 6,
        out_specs=(full(), full()),
        name="bucket",
    )(*[owner.reshape(1, -1) for owner in owners], *rows)

    arrived = exchange(requests)
    chunk = nodes // 16
    group = devices // PARTS
    located = pl.pallas_call(
        functools.partial(gather_kernel, slots, chunk, group),
        out_shape=jax.ShapeDtypeStruct((devices, held, LANES), BF16),
        in_specs=[full(pl.ANY), full(pl.ANY)],
        out_specs=full(pl.ANY),
        scratch_shapes=[
            pltpu.SMEM(arrived.shape, jnp.int32),
            pltpu.VMEM((nodes, width), BF16),
            pltpu.VMEM((2 * nodes, LANES), F32),
            pltpu.VMEM((stride, LANES), F32),
            pltpu.VMEM((devices, held, LANES), BF16),
            pltpu.SemaphoreType.DMA,
            pltpu.SemaphoreType.DMA((nodes // chunk,)),
            pltpu.SemaphoreType.DMA((PARTS,)),
        ],
        name="owner_gather",
    )(arrived, features)
    returned = exchange(located)

    share1 = mean_shares(hop1_rel.reshape(counts[0], FAN1))
    share2 = mean_shares(hop2_rel.reshape(counts[1], FAN2))
    positives = edge_mask.shape[0]
    loss, sums = pl.pallas_call(
        functools.partial(model_kernel, counts, stride, group),
        out_shape=(
            jax.ShapeDtypeStruct((1, positives), F32),
            jax.ShapeDtypeStruct((devices, 1, LANES), F32),
        ),
        in_specs=[full(pl.ANY)] * 4 + [full()] * 3,
        out_specs=(full(), full()),
        scratch_shapes=[
            pltpu.SMEM((blocks, LANES), jnp.int32),
            pltpu.VMEM((devices, held, LANES), BF16),
            pltpu.VMEM(w_first.shape, BF16),
            pltpu.VMEM(w_second.shape, BF16),
            pltpu.VMEM((devices * stride, LANES), F32),
        ]
        + [pltpu.VMEM((2 * count, LANES), F32) for count in counts]
        + [pltpu.VMEM((counts[1], LANES), F32)] * 2
        + [pltpu.SemaphoreType.DMA((3,)), pltpu.SemaphoreType.DMA((PARTS,))],
        name="model",
    )(places, returned, w_first, w_second, share1, share2, edge_mask.reshape(1, -1))
    totals = jnp.sum(exchange(sums), axis=(0, 1))
    mean_loss = totals[0] / jnp.maximum(totals[1], 1.0)
    return (loss.reshape(positives), mean_loss)


def solution(mesh):
    placed = (
        P("dom", None), P(), P(), P("dom", None), P("dom"), P("dom", None), P("dom"), P("dom"),
        P("dom", None), P("dom"), P("dom"), P("dom"),
    )
    return jax.shard_map(
        shards, mesh=mesh, in_specs=placed, out_specs=(P("dom"), P()), check_vma=False
    )
```

```python
import functools

import jax
import jax.numpy as jnp
from jax import lax
from jax.experimental import pallas as pl
from jax.experimental.pallas import tpu as pltpu
from jax.sharding import PartitionSpec as P

R = 4
BLOCK = 128
NEG = 32
FAN1 = 4
FAN2 = 2
LANES = 128
PARTS = 4
HOP_STEP = 384
F32 = jnp.float32
BF16 = jnp.bfloat16
HIGHEST = lax.Precision.HIGHEST


def round_up(value, unit):
    return (value + unit - 1) // unit * unit


def full(memory_space=pltpu.VMEM):
    return pl.BlockSpec(memory_space=memory_space)


def bucket_kernel(offsets, stride, counts, *refs):
    kinds = len(counts)
    owner_refs, row_refs = refs[:kinds], refs[kinds : 2 * kinds]
    request_ref, slot_ref, hots, ranks, halves, spread = refs[2 * kinds :]
    devices, _, width = request_ref.shape
    device = lax.broadcasted_iota(jnp.int32, (devices, LANES), 0)
    before = lax.broadcasted_iota(jnp.int32, (LANES, 2 * LANES), 0)
    lane = lax.broadcasted_iota(jnp.int32, (LANES, 2 * LANES), 1)
    earlier = jnp.where(before < lane, 1.0, 0.0).astype(BF16)
    place = lax.broadcasted_iota(jnp.int32, (width, LANES), 0)
    entries = []
    for kind, count in enumerate(counts):
        for start in range(0, count, LANES):
            size = min(LANES, count - start)
            owner = owner_refs[kind][:, start : start + size]
            row = row_refs[kind][pl.ds(start, size)].reshape(1, size)
            if size < LANES:
                owner = jnp.concatenate([owner, jnp.full((1, LANES - size), -1, jnp.int32)], axis=1)
                row = jnp.concatenate([row, jnp.zeros((1, LANES - size), jnp.int32)], axis=1)
            hot = jnp.where(device == owner, 1.0, 0.0)
            block = len(entries)
            hots[block * devices : (block + 1) * devices, :] = hot.astype(BF16)
            span = slice(block * LANES, (block + 1) * LANES)
            halves[:devices, span] = (hot * (row // LANES).astype(F32)).astype(BF16)
            halves[devices:, span] = (hot * (row % LANES).astype(F32)).astype(BF16)
            entries.append((kind, owner, hot))
    ranks[...] = jnp.dot(hots[...], earlier, preferred_element_type=F32)
    carried, current = None, None
    for block, (kind, owner, hot) in enumerate(entries):
        if kind != current:
            carried, current = jnp.zeros((devices, LANES), F32), kind
        span = slice(block * devices, (block + 1) * devices)
        prior = ranks[span, :LANES] + carried
        carried = carried + ranks[span, LANES:]
        position = jnp.sum(hot * prior, axis=0, keepdims=True).astype(jnp.int32) + offsets[kind]
        slot_ref[block : block + 1, :] = jnp.maximum(owner, 0) * stride + 2 * position
        spread[:, block * LANES : (block + 1) * LANES] = jnp.where(
            place == position, 1.0, 0.0
        ).astype(BF16)
    total = lax.dot_general(
        halves[...], spread[...], (((1,), (1,)), ((), ())), preferred_element_type=F32
    )
    request = (total[:devices] * (2.0 * LANES) + total[devices:] * 2.0).astype(jnp.int32)
    request_ref[...] = request.reshape(devices, 1, width)


def gather_kernel(
    slots, chunk, group, request_ref, table_ref, out_ref, request, staged, wide, packed, rows_out,
    request_sem, sems, out_sems,
):
    devices = out_ref.shape[0]
    pieces = table_ref.shape[0] // chunk
    asked = pltpu.make_async_copy(request_ref, request, request_sem)
    asked.start()

    def copy(piece):
        span = pl.ds(piece * chunk, chunk)
        return pltpu.make_async_copy(table_ref.at[span], staged.at[span], sems.at[piece])

    for piece in range(pieces):
        copy(piece).start()
    step = min(chunk, 256)
    for piece in range(pieces):
        copy(piece).wait()

        def widen(index, _):
            base = pl.multiple_of(piece * chunk + index * step, step)
            values = staged[pl.ds(base, step), :].astype(F32)
            wide[pl.ds(2 * base, step, stride=2), :] = values[:, :LANES]
            wide[pl.ds(2 * base + 1, step, stride=2), :] = values[:, LANES:]
            return 0

        lax.fori_loop(0, chunk // step, widen, 0)
    asked.wait()

    def serve(device, _):
        for slot in range(slots):
            row = pl.multiple_of(request[device, 0, slot], 2)
            packed[pl.ds(2 * slot, 2), :] = wide[pl.ds(row, 2), :]
        rows_out[device] = packed[: 2 * slots, :].astype(BF16)
        return 0

    def leave(part):
        span = pl.ds(part * group, group)
        return pltpu.make_async_copy(rows_out.at[span], out_ref.at[span], out_sems.at[part])

    for part in range(devices // group):
        for device in range(part * group, (part + 1) * group):
            serve(device, 0)
        leave(part).start()
    for part in range(devices // group):
        leave(part).wait()


def layer(selves, neighbours, share, weights):
    pieces = list(selves)
    fan = len(neighbours)
    for relation in range(R):
        for half in range(2):
            merged = share(relation, 0) * neighbours[0][half]
            for k in range(1, fan):
                merged = merged + share(relation, k) * neighbours[k][half]
            pieces.append(merged)
    inputs = jnp.concatenate([piece.astype(BF16) for piece in pieces], axis=1)
    return jnp.dot(inputs, weights, preferred_element_type=F32)


def model_kernel(
    counts, stride, group, slot_hbm, got_hbm, first_hbm, second_hbm, share1_hbm, share2_hbm, mask_hbm,
    loss_ref, sums_ref, slot_ref, got, first_ref, second_ref, share1_ref, share2_ref, mask_ref, wide, x0, x1, x2, h_low, h_high, sems,
    got_sems,
):
    devices, held, _ = got_hbm.shape
    seeds, firsts, _ = counts

    def arrive(part):
        span = pl.ds(part * group, group)
        return pltpu.make_async_copy(got_hbm.at[span], got.at[span], got_sems.at[part])

    for part in range(devices // group):
        arrive(part).start()
    side = [
        pltpu.make_async_copy(source, target, sems.at[number])
        for number, (source, target) in enumerate(
            (
                (slot_hbm, slot_ref), (first_hbm, first_ref), (share2_hbm, share2_ref),
                (share1_hbm, share1_ref), (second_hbm, second_ref), (mask_hbm, mask_ref),
            )
        )
    ]
    for copy in side:
        copy.start()

    def widen(device, _):
        wide[pl.ds(pl.multiple_of(device * stride, 8), held), :] = got[device].astype(F32)
        return 0

    for part in range(devices // group):
        arrive(part).wait()
        lax.fori_loop(part * group, (part + 1) * group, widen, 0)
    side[0].wait()
    block = 0
    for target, count in zip((x0, x1, x2), counts):
        whole = count // LANES

        for item in range(count):
            slot = pl.multiple_of(slot_ref[block + item // LANES, item % LANES], 2)
            target[pl.ds(2 * item, 2), :] = wide[pl.ds(slot, 2), :]
        block += -(-count // LANES)

    step = HOP_STEP
    side[1].wait()
    side[2].wait()
    side[3].wait()
    side[4].wait()
    side[5].wait()

    def hop(index, _):
        base = pl.multiple_of(index * step, step)
        selves = [x1[pl.ds(2 * base + half, step, stride=2), :] for half in range(2)]
        neighbours = [
            [x2[pl.ds(2 * FAN2 * base + 2 * k + half, step, stride=2 * FAN2), :] for half in range(2)]
            for k in range(FAN2)
        ]
        shares = share2_ref[pl.ds(base, step), :]
        hidden = layer(
            selves, neighbours, lambda r, k: shares[:, r * FAN2 + k : r * FAN2 + k + 1], first_ref[...]
        )
        hidden = jnp.maximum(hidden, 0.0).astype(BF16).astype(F32)
        h_low[pl.ds(base, step), :] = hidden[:, :LANES]
        h_high[pl.ds(base, step), :] = hidden[:, LANES:]
        return 0

    lax.fori_loop(0, firsts // step, hop, 0)
    shares = share1_ref[...]
    share = lambda r, k: shares[:, r * FAN1 + k : r * FAN1 + k + 1]
    selves = [x0[pl.ds(half, seeds, stride=2), :] for half in range(2)]
    neighbours = [
        [x1[pl.ds(2 * k + half, seeds, stride=2 * FAN1), :] for half in range(2)] for k in range(FAN1)
    ]
    hidden = jnp.maximum(layer(selves, neighbours, share, first_ref[...]), 0.0).astype(BF16)
    selves = [hidden[:, :LANES], hidden[:, LANES:]]
    neighbours = [
        [h[pl.ds(k, seeds, stride=FAN1), :] for h in (h_low, h_high)] for k in range(FAN1)
    ]
    second = layer(selves, neighbours, share, second_ref[...])
    positives = mask_ref.shape[1]
    width = second.shape[1]
    contract = (((1,), (1,)), ((), ()))
    loss_sum = jnp.zeros((1, 1), F32)
    for number in range(positives // BLOCK):
        span = slice(number * BLOCK, (number + 1) * BLOCK)
        sources = second[span]
        targets = second[positives + number * BLOCK : positives + (number + 1) * BLOCK]
        negatives = second[2 * positives + number * NEG : 2 * positives + (number + 1) * NEG]
        positive = lax.dot_general(
            jnp.ones((8, width), F32), sources * targets, contract, precision=HIGHEST,
            preferred_element_type=F32,
        )[:1]
        negative = lax.dot_general(
            negatives, sources, contract, precision=HIGHEST, preferred_element_type=F32
        )
        top = jnp.maximum(jnp.max(negative, axis=0, keepdims=True), positive)
        spread = jnp.sum(jnp.exp(negative - top), axis=0, keepdims=True) + jnp.exp(positive - top)
        loss = top + jnp.log(spread) - positive
        loss_ref[:, span] = loss
        loss_sum = loss_sum + jnp.sum(
            mask_ref[:, span].astype(F32) * loss, axis=1, keepdims=True
        )
    edge_sum = jnp.sum(mask_ref[...].astype(F32), axis=1, keepdims=True)
    lane = lax.broadcasted_iota(jnp.int32, (devices, 1, LANES), 2)
    sums_ref[...] = jnp.where(
        lane == 0, loss_sum.reshape(1, 1, 1), jnp.where(lane == 1, edge_sum.reshape(1, 1, 1), 0.0)
    )


def mean_shares(relations):
    onehot = (relations[..., None] == jnp.arange(R, dtype=jnp.int32)).astype(F32)
    tallies = jnp.maximum(jnp.sum(onehot, axis=1), 1.0)
    shares = onehot / tallies[:, None, :]
    return jnp.transpose(shares, (0, 2, 1)).reshape(relations.shape[0], -1)


def exchange(array):
    return lax.all_to_all(array, "dom", split_axis=0, concat_axis=0, tiled=True)


def shards(
    features, w_first, w_second, seed_owner, seed_row, hop1_owner, hop1_row, hop1_rel,
    hop2_owner, hop2_row, hop2_rel, edge_mask,
):
    devices = lax.axis_size("dom")
    nodes, width = features.shape
    owners = (seed_owner, hop1_owner, hop2_owner)
    rows = (seed_row, hop1_row, hop2_row)
    counts = tuple(row.shape[0] for row in rows)
    capacities = [(2 * count + devices - 1) // devices for count in counts]
    offsets = [sum(capacities[:kind]) for kind in range(len(counts))]
    slots = sum(capacities)
    held = 2 * slots
    stride = round_up(held, 8)
    blocks = sum(-(-count // LANES) for count in counts)

    requests, places = pl.pallas_call(
        functools.partial(bucket_kernel, offsets, stride, counts),
        out_shape=(
            pltpu.VMEM((devices, 1, round_up(slots, LANES)), jnp.int32),
            jax.ShapeDtypeStruct((blocks, LANES), jnp.int32),
        ),
        in_specs=[full()] * 6,
        out_specs=(full(), full()),
        scratch_shapes=[
            pltpu.VMEM((blocks * devices, LANES), BF16),
            pltpu.VMEM((blocks * devices, 2 * LANES), F32),
            pltpu.VMEM((2 * devices, blocks * LANES), BF16),
            pltpu.VMEM((round_up(slots, LANES), blocks * LANES), BF16),
        ],
        name="bucket",
    )(*[owner.reshape(1, -1) for owner in owners], *rows)

    arrived = exchange(requests)
    chunk = nodes // 16
    group = devices // PARTS
    located = pl.pallas_call(
        functools.partial(gather_kernel, slots, chunk, group),
        out_shape=jax.ShapeDtypeStruct((devices, held, LANES), BF16),
        in_specs=[full(pl.ANY), full(pl.ANY)],
        out_specs=full(pl.ANY),
        scratch_shapes=[
            pltpu.SMEM(arrived.shape, jnp.int32),
            pltpu.VMEM((nodes, width), BF16),
            pltpu.VMEM((2 * nodes, LANES), F32),
            pltpu.VMEM((stride, LANES), F32),
            pltpu.VMEM((devices, held, LANES), BF16),
            pltpu.SemaphoreType.DMA,
            pltpu.SemaphoreType.DMA((nodes // chunk,)),
            pltpu.SemaphoreType.DMA((PARTS,)),
        ],
        name="owner_gather",
    )(arrived, features)
    returned = exchange(located)

    share1 = mean_shares(hop1_rel.reshape(counts[0], FAN1))
    share2 = mean_shares(hop2_rel.reshape(counts[1], FAN2))
    positives = edge_mask.shape[0]
    loss, sums = pl.pallas_call(
        functools.partial(model_kernel, counts, stride, group),
        out_shape=(
            jax.ShapeDtypeStruct((1, positives), F32),
            pltpu.VMEM((devices, 1, LANES), F32),
        ),
        in_specs=[full(pl.ANY)] * 7,
        out_specs=(full(), full()),
        scratch_shapes=[
            pltpu.SMEM((blocks, LANES), jnp.int32),
            pltpu.VMEM((devices, held, LANES), BF16),
            pltpu.VMEM(w_first.shape, BF16),
            pltpu.VMEM(w_second.shape, BF16),
            pltpu.VMEM(share1.shape, F32),
            pltpu.VMEM(share2.shape, F32),
            pltpu.VMEM((1, positives), jnp.int32),
            pltpu.VMEM((devices * stride, LANES), F32),
        ]
        + [pltpu.VMEM((2 * count, LANES), F32) for count in counts]
        + [pltpu.VMEM((counts[1], LANES), F32)] * 2
        + [pltpu.SemaphoreType.DMA((6,)), pltpu.SemaphoreType.DMA((PARTS,))],
        name="model",
    )(places, returned, w_first, w_second, share1, share2, edge_mask.reshape(1, -1))
    totals = jnp.sum(exchange(sums), axis=(0, 1))
    mean_loss = totals[0] / jnp.maximum(totals[1], 1.0)
    return (loss.reshape(positives), mean_loss)


def solution(mesh):
    placed = (
        P("dom", None), P(), P(), P("dom", None), P("dom"), P("dom", None), P("dom"), P("dom"),
        P("dom", None), P("dom"), P("dom"), P("dom"),
    )
    return jax.shard_map(
        shards, mesh=mesh, in_specs=placed, out_specs=(P("dom"), P()), check_vma=False
    )
```

```python
import functools

import jax
import jax.numpy as jnp
from jax import lax
from jax.experimental import pallas as pl
from jax.experimental.pallas import tpu as pltpu
from jax.sharding import PartitionSpec as P

R = 4
BLOCK = 128
NEG = 32
FAN1 = 4
FAN2 = 2
LANES = 128
PARTS = 4
HOP_STEP = 128
F32 = jnp.float32
BF16 = jnp.bfloat16
HIGHEST = lax.Precision.HIGHEST


def round_up(value, unit):
    return (value + unit - 1) // unit * unit


def full(memory_space=pltpu.VMEM):
    return pl.BlockSpec(memory_space=memory_space)


def bucket_kernel(offsets, stride, counts, *refs):
    kinds = len(counts)
    owner_refs, row_refs = refs[:kinds], refs[kinds : 2 * kinds]
    request_ref, slot_ref, hots, ranks, halves, spread = refs[2 * kinds :]
    devices, _, width = request_ref.shape
    device = lax.broadcasted_iota(jnp.int32, (devices, LANES), 0)
    before = lax.broadcasted_iota(jnp.int32, (LANES, 2 * LANES), 0)
    lane = lax.broadcasted_iota(jnp.int32, (LANES, 2 * LANES), 1)
    earlier = jnp.where(before < lane, 1.0, 0.0).astype(BF16)
    place = lax.broadcasted_iota(jnp.int32, (width, LANES), 0)
    entries = []
    for kind, count in enumerate(counts):
        for start in range(0, count, LANES):
            size = min(LANES, count - start)
            owner = owner_refs[kind][:, start : start + size]
            row = row_refs[kind][pl.ds(start, size)].reshape(1, size)
            if size < LANES:
                owner = jnp.concatenate([owner, jnp.full((1, LANES - size), -1, jnp.int32)], axis=1)
                row = jnp.concatenate([row, jnp.zeros((1, LANES - size), jnp.int32)], axis=1)
            hot = jnp.where(device == owner, 1.0, 0.0)
            block = len(entries)
            hots[block * devices : (block + 1) * devices, :] = hot.astype(BF16)
            span = slice(block * LANES, (block + 1) * LANES)
            halves[:devices, span] = (hot * (row // LANES).astype(F32)).astype(BF16)
            halves[devices:, span] = (hot * (row % LANES).astype(F32)).astype(BF16)
            entries.append((kind, owner, hot))
    ranks[...] = jnp.dot(hots[...], earlier, preferred_element_type=F32)
    carried, current = None, None
    for block, (kind, owner, hot) in enumerate(entries):
        if kind != current:
            carried, current = jnp.zeros((devices, LANES), F32), kind
        span = slice(block * devices, (block + 1) * devices)
        prior = ranks[span, :LANES] + carried
        carried = carried + ranks[span, LANES:]
        position = jnp.sum(hot * prior, axis=0, keepdims=True).astype(jnp.int32) + offsets[kind]
        slot_ref[block : block + 1, :] = jnp.maximum(owner, 0) * stride + 2 * position
        spread[:, block * LANES : (block + 1) * LANES] = jnp.where(
            place == position, 1.0, 0.0
        ).astype(BF16)
    total = lax.dot_general(
        halves[...], spread[...], (((1,), (1,)), ((), ())), preferred_element_type=F32
    )
    request = (total[:devices] * (2.0 * LANES) + total[devices:] * 2.0).astype(jnp.int32)
    request_ref[...] = request.reshape(devices, 1, width)


def gather_kernel(
    slots, chunk, group, request_ref, table_ref, out_ref, request, staged, wide, packed, rows_out,
    request_sem, sems, out_sems,
):
    devices = out_ref.shape[0]
    pieces = table_ref.shape[0] // chunk
    asked = pltpu.make_async_copy(request_ref, request, request_sem)
    asked.start()

    def copy(piece):
        span = pl.ds(piece * chunk, chunk)
        return pltpu.make_async_copy(table_ref.at[span], staged.at[span], sems.at[piece])

    for piece in range(pieces):
        copy(piece).start()
    step = min(chunk, 256)
    for piece in range(pieces):
        copy(piece).wait()

        def widen(index, _):
            base = pl.multiple_of(piece * chunk + index * step, step)
            values = staged[pl.ds(base, step), :].astype(F32)
            wide[pl.ds(2 * base, step, stride=2), :] = values[:, :LANES]
            wide[pl.ds(2 * base + 1, step, stride=2), :] = values[:, LANES:]
            return 0

        lax.fori_loop(0, chunk // step, widen, 0)
    asked.wait()

    def serve(device, _):
        for slot in range(slots):
            row = pl.multiple_of(request[device, 0, slot], 2)
            packed[pl.ds(2 * slot, 2), :] = wide[pl.ds(row, 2), :]
        rows_out[device] = packed[: 2 * slots, :].astype(BF16)
        return 0

    def leave(part):
        span = pl.ds(part * group, group)
        return pltpu.make_async_copy(rows_out.at[span], out_ref.at[span], out_sems.at[part])

    for part in range(devices // group):
        for device in range(part * group, (part + 1) * group):
            serve(device, 0)
        leave(part).start()
    for part in range(devices // group):
        leave(part).wait()


def layer(selves, neighbours, share, weights):
    pieces = list(selves)
    fan = len(neighbours)
    for relation in range(R):
        for half in range(2):
            merged = share(relation, 0) * neighbours[0][half]
            for k in range(1, fan):
                merged = merged + share(relation, k) * neighbours[k][half]
            pieces.append(merged)
    inputs = jnp.concatenate([piece.astype(BF16) for piece in pieces], axis=1)
    return jnp.dot(inputs, weights, preferred_element_type=F32)


def model_kernel(
    counts, stride, split, slot_hbm, got_hbm, first_hbm, second_hbm, share1_hbm, share2_hbm, mask_hbm,
    loss_ref, sums_ref, slot_ref, got, first_ref, second_ref, share1_ref, share2_ref, mask_ref, wide, x0, x1, x2, h_low, h_high, sems,
    got_sems,
):
    devices, held, _ = got_hbm.shape
    seeds, firsts, _ = counts

    bounds = ((0, split), (split, held))

    def arrive(half):
        span = pl.ds(bounds[half][0], bounds[half][1] - bounds[half][0])
        return pltpu.make_async_copy(got_hbm.at[:, span], got.at[:, span], got_sems.at[half])

    side = [
        pltpu.make_async_copy(source, target, sems.at[number])
        for number, (source, target) in enumerate(
            (
                (slot_hbm, slot_ref), (first_hbm, first_ref), (share2_hbm, share2_ref),
                (share1_hbm, share1_ref), (second_hbm, second_ref), (mask_hbm, mask_ref),
            )
        )
    ]
    side[0].start()
    for half in range(2):
        arrive(half).start()
    for copy in side[1:]:
        copy.start()

    def take(half):
        arrive(half).wait()
        start, end = bounds[half]

        def widen(device, _):
            base = pl.multiple_of(device * stride, 8) + start
            wide[pl.ds(pl.multiple_of(base, 8), end - start), :] = got[
                device, start:end, :
            ].astype(F32)
            return 0

        lax.fori_loop(0, devices, widen, 0)

    side[0].wait()
    take(0)
    firsts_block = -(-seeds // LANES)
    seconds_block = firsts_block + -(-firsts // LANES)

    def fetch(target, block, start, end):
        for item in range(start, end):
            slot = pl.multiple_of(slot_ref[block + item // LANES, item % LANES], 2)
            target[pl.ds(2 * item, 2), :] = wide[pl.ds(slot, 2), :]

    step = HOP_STEP
    fetch(x0, 0, 0, seeds)
    fetch(x1, firsts_block, 0, firsts)
    take(1)
    for number in range(1, len(side)):
        side[number].wait()

    for base in range(0, firsts, step):
        fetch(x2, seconds_block, FAN2 * base, FAN2 * (base + step))
        selves = [x1[pl.ds(2 * base + half, step, stride=2), :] for half in range(2)]
        neighbours = [
            [x2[pl.ds(2 * FAN2 * base + 2 * k + half, step, stride=2 * FAN2), :] for half in range(2)]
            for k in range(FAN2)
        ]
        shares2 = share2_ref[base : base + step, :]
        hidden = layer(
            selves, neighbours,
            lambda r, k, shares2=shares2: shares2[:, r * FAN2 + k : r * FAN2 + k + 1],
            first_ref[...],
        )
        hidden = jnp.maximum(hidden, 0.0).astype(BF16).astype(F32)
        h_low[base : base + step, :] = hidden[:, :LANES]
        h_high[base : base + step, :] = hidden[:, LANES:]

    shares = share1_ref[...]
    share = lambda r, k: shares[:, r * FAN1 + k : r * FAN1 + k + 1]
    selves = [x0[pl.ds(half, seeds, stride=2), :] for half in range(2)]
    neighbours = [
        [x1[pl.ds(2 * k + half, seeds, stride=2 * FAN1), :] for half in range(2)] for k in range(FAN1)
    ]
    hidden = jnp.maximum(layer(selves, neighbours, share, first_ref[...]), 0.0).astype(BF16)
    selves = [hidden[:, :LANES], hidden[:, LANES:]]
    neighbours = [
        [h[pl.ds(k, seeds, stride=FAN1), :] for h in (h_low, h_high)] for k in range(FAN1)
    ]
    second = layer(selves, neighbours, share, second_ref[...])
    positives = mask_ref.shape[1]
    width = second.shape[1]
    contract = (((1,), (1,)), ((), ()))
    loss_sum = jnp.zeros((1, 1), F32)
    for number in range(positives // BLOCK):
        span = slice(number * BLOCK, (number + 1) * BLOCK)
        sources = second[span]
        targets = second[positives + number * BLOCK : positives + (number + 1) * BLOCK]
        negatives = second[2 * positives + number * NEG : 2 * positives + (number + 1) * NEG]
        positive = lax.dot_general(
            jnp.ones((8, width), F32), sources * targets, contract, precision=HIGHEST,
            preferred_element_type=F32,
        )[:1]
        negative = lax.dot_general(
            negatives, sources, contract, precision=HIGHEST, preferred_element_type=F32
        )
        top = jnp.maximum(jnp.max(negative, axis=0, keepdims=True), positive)
        spread = jnp.sum(jnp.exp(negative - top), axis=0, keepdims=True) + jnp.exp(positive - top)
        loss = top + jnp.log(spread) - positive
        loss_ref[:, span] = loss
        loss_sum = loss_sum + jnp.sum(
            mask_ref[:, span].astype(F32) * loss, axis=1, keepdims=True
        )
    edge_sum = jnp.sum(mask_ref[...].astype(F32), axis=1, keepdims=True)
    lane = lax.broadcasted_iota(jnp.int32, (devices, 1, LANES), 2)
    sums_ref[...] = jnp.where(
        lane == 0, loss_sum.reshape(1, 1, 1), jnp.where(lane == 1, edge_sum.reshape(1, 1, 1), 0.0)
    )


def mean_kernel(sums_ref, mean_ref):
    totals = jnp.sum(sums_ref[...], axis=0)
    mean_ref[...] = totals[:, :1] / jnp.maximum(totals[:, 1:2], 1.0)


def mean_shares(relations):
    onehot = (relations[..., None] == jnp.arange(R, dtype=jnp.int32)).astype(F32)
    tallies = jnp.maximum(jnp.sum(onehot, axis=1), 1.0)
    shares = onehot / tallies[:, None, :]
    return jnp.transpose(shares, (0, 2, 1)).reshape(relations.shape[0], -1)


def exchange(array):
    return lax.all_to_all(array, "dom", split_axis=0, concat_axis=0, tiled=True)


def shards(
    features, w_first, w_second, seed_owner, seed_row, hop1_owner, hop1_row, hop1_rel,
    hop2_owner, hop2_row, hop2_rel, edge_mask,
):
    devices = lax.axis_size("dom")
    nodes, width = features.shape
    owners = (seed_owner, hop1_owner, hop2_owner)
    rows = (seed_row, hop1_row, hop2_row)
    counts = tuple(row.shape[0] for row in rows)
    capacities = [(2 * count + devices - 1) // devices for count in counts]
    offsets = [sum(capacities[:kind]) for kind in range(len(counts))]
    slots = sum(capacities)
    held = 2 * slots
    stride = round_up(held, 8)
    blocks = sum(-(-count // LANES) for count in counts)

    requests, places = pl.pallas_call(
        functools.partial(bucket_kernel, offsets, stride, counts),
        out_shape=(
            pltpu.VMEM((devices, 1, round_up(slots, LANES)), jnp.int32),
            pltpu.VMEM((blocks, LANES), jnp.int32),
        ),
        in_specs=[full()] * 6,
        out_specs=(full(), full()),
        scratch_shapes=[
            pltpu.VMEM((blocks * devices, LANES), BF16),
            pltpu.VMEM((blocks * devices, 2 * LANES), F32),
            pltpu.VMEM((2 * devices, blocks * LANES), BF16),
            pltpu.VMEM((round_up(slots, LANES), blocks * LANES), BF16),
        ],
        name="bucket",
    )(*[owner.reshape(1, -1) for owner in owners], *rows)

    arrived = exchange(requests)
    chunk = nodes // 16
    group = devices // PARTS
    located = pl.pallas_call(
        functools.partial(gather_kernel, slots, chunk, group),
        out_shape=jax.ShapeDtypeStruct((devices, held, LANES), BF16),
        in_specs=[full(pl.ANY), full(pl.ANY)],
        out_specs=full(pl.ANY),
        scratch_shapes=[
            pltpu.SMEM(arrived.shape, jnp.int32),
            pltpu.VMEM((nodes, width), BF16),
            pltpu.VMEM((2 * nodes, LANES), F32),
            pltpu.VMEM((stride, LANES), F32),
            pltpu.VMEM((devices, held, LANES), BF16),
            pltpu.SemaphoreType.DMA,
            pltpu.SemaphoreType.DMA((nodes // chunk,)),
            pltpu.SemaphoreType.DMA((PARTS,)),
        ],
        name="owner_gather",
    )(arrived, features)
    returned = exchange(located)

    share1 = mean_shares(hop1_rel.reshape(counts[0], FAN1))
    share2 = mean_shares(hop2_rel.reshape(counts[1], FAN2))
    positives = edge_mask.shape[0]
    loss, sums = pl.pallas_call(
        functools.partial(model_kernel, counts, stride, round_up(2 * offsets[2], 8)),
        out_shape=(
            pltpu.VMEM((1, positives), F32),
            pltpu.VMEM((devices, 1, LANES), F32),
        ),
        in_specs=[full(pl.ANY)] * 7,
        out_specs=(full(), full()),
        scratch_shapes=[
            pltpu.SMEM((blocks, LANES), jnp.int32),
            pltpu.VMEM((devices, held, LANES), BF16),
            pltpu.VMEM(w_first.shape, BF16),
            pltpu.VMEM(w_second.shape, BF16),
            pltpu.VMEM(share1.shape, F32),
            pltpu.VMEM(share2.shape, F32),
            pltpu.VMEM((1, positives), jnp.int32),
            pltpu.VMEM((devices * stride, LANES), F32),
        ]
        + [pltpu.VMEM((2 * count, LANES), F32) for count in counts]
        + [pltpu.VMEM((counts[1], LANES), F32)] * 2
        + [pltpu.SemaphoreType.DMA((6,)), pltpu.SemaphoreType.DMA((2,))],
        name="model",
    )(places, returned, w_first, w_second, share1, share2, edge_mask.reshape(1, -1))
    mean_loss = pl.pallas_call(
        mean_kernel,
        out_shape=jax.ShapeDtypeStruct((1, 1), F32),
        in_specs=[full()],
        out_specs=full(),
        compiler_params=pltpu.CompilerParams(vmem_limit_bytes=2**20),
        name="mean",
    )(exchange(sums))
    return (loss.reshape(positives), mean_loss.reshape(()))


def solution(mesh):
    placed = (
        P("dom", None), P(), P(), P("dom", None), P("dom"), P("dom", None), P("dom"), P("dom"),
        P("dom", None), P("dom"), P("dom"), P("dom"),
    )
    return jax.shard_map(
        shards, mesh=mesh, in_specs=placed, out_specs=(P("dom"), P()), check_vma=False
    )
```

```python
import functools

import jax
import jax.numpy as jnp
from jax import lax
from jax.experimental import pallas as pl
from jax.experimental.pallas import tpu as pltpu
from jax.sharding import PartitionSpec as P

R = 4
BLOCK = 128
NEG = 32
FAN1 = 4
FAN2 = 2
LANES = 128
PARTS = 8
HOP_STEP = 128
F32 = jnp.float32
BF16 = jnp.bfloat16
HIGHEST = lax.Precision.HIGHEST


def round_up(value, unit):
    return (value + unit - 1) // unit * unit


def full(memory_space=pltpu.VMEM):
    return pl.BlockSpec(memory_space=memory_space)


def bucket_kernel(offsets, stride, counts, *refs):
    kinds = len(counts)
    owner_refs, row_refs = refs[:kinds], refs[kinds : 2 * kinds]
    request_ref, slot_ref, hots, ranks, halves, spread = refs[2 * kinds :]
    devices, _, width = request_ref.shape
    device = lax.broadcasted_iota(jnp.int32, (devices, LANES), 0)
    before = lax.broadcasted_iota(jnp.int32, (LANES, 2 * LANES), 0)
    lane = lax.broadcasted_iota(jnp.int32, (LANES, 2 * LANES), 1)
    earlier = jnp.where(before < lane, 1.0, 0.0).astype(BF16)
    place = lax.broadcasted_iota(jnp.int32, (width, LANES), 0)
    entries = []
    for kind, count in enumerate(counts):
        for start in range(0, count, LANES):
            size = min(LANES, count - start)
            owner = owner_refs[kind][:, start : start + size]
            row = row_refs[kind][pl.ds(start, size)].reshape(1, size)
            if size < LANES:
                owner = jnp.concatenate([owner, jnp.full((1, LANES - size), -1, jnp.int32)], axis=1)
                row = jnp.concatenate([row, jnp.zeros((1, LANES - size), jnp.int32)], axis=1)
            hot = jnp.where(device == owner, 1.0, 0.0)
            block = len(entries)
            hots[block * devices : (block + 1) * devices, :] = hot.astype(BF16)
            span = slice(block * LANES, (block + 1) * LANES)
            halves[:devices, span] = (hot * (row // LANES).astype(F32)).astype(BF16)
            halves[devices:, span] = (hot * (row % LANES).astype(F32)).astype(BF16)
            entries.append((kind, owner, hot))
    ranks[...] = jnp.dot(hots[...], earlier, preferred_element_type=F32)
    carried, current = None, None
    for block, (kind, owner, hot) in enumerate(entries):
        if kind != current:
            carried, current = jnp.zeros((devices, LANES), F32), kind
        span = slice(block * devices, (block + 1) * devices)
        prior = ranks[span, :LANES] + carried
        carried = carried + ranks[span, LANES:]
        position = jnp.sum(hot * prior, axis=0, keepdims=True).astype(jnp.int32) + offsets[kind]
        slot_ref[block : block + 1, :] = jnp.maximum(owner, 0) * stride + 2 * position
        spread[:, block * LANES : (block + 1) * LANES] = jnp.where(
            place == position, 1.0, 0.0
        ).astype(BF16)
    total = lax.dot_general(
        halves[...], spread[...], (((1,), (1,)), ((), ())), preferred_element_type=F32
    )
    request = (total[:devices] * (2.0 * LANES) + total[devices:] * 2.0).astype(jnp.int32)
    request_ref[...] = request.reshape(devices, 1, width)


def gather_kernel(
    slots, chunk, group, request_ref, table_ref, out_ref, request, staged, wide, packed, rows_out,
    request_sem, sems, out_sems,
):
    devices = out_ref.shape[0]
    pieces = table_ref.shape[0] // chunk
    asked = pltpu.make_async_copy(request_ref, request, request_sem)
    asked.start()

    def copy(piece):
        span = pl.ds(piece * chunk, chunk)
        return pltpu.make_async_copy(table_ref.at[span], staged.at[span], sems.at[piece])

    for piece in range(pieces):
        copy(piece).start()
    step = min(chunk, 256)
    for piece in range(pieces):
        copy(piece).wait()

        def widen(index, _):
            base = pl.multiple_of(piece * chunk + index * step, step)
            values = staged[pl.ds(base, step), :].astype(F32)
            wide[pl.ds(2 * base, step, stride=2), :] = values[:, :LANES]
            wide[pl.ds(2 * base + 1, step, stride=2), :] = values[:, LANES:]
            return 0

        lax.fori_loop(0, chunk // step, widen, 0)
    asked.wait()

    def serve(device):
        turn = packed.at[device % 2]
        for slot in range(slots):
            row = pl.multiple_of(request[device, 0, slot], 2)
            turn[pl.ds(2 * slot, 2), :] = wide[pl.ds(row, 2), :]
        rows_out[device] = turn[: 2 * slots, :].astype(BF16)

    def leave(part):
        span = pl.ds(part * group, group)
        return pltpu.make_async_copy(rows_out.at[span], out_ref.at[span], out_sems.at[part])

    for part in range(devices // group):
        for device in range(part * group, (part + 1) * group):
            serve(device)
        leave(part).start()
    for part in range(devices // group):
        leave(part).wait()


def layer(selves, neighbours, share, weights):
    pieces = list(selves)
    fan = len(neighbours)
    for relation in range(R):
        for half in range(2):
            merged = share(relation, 0) * neighbours[0][half]
            for k in range(1, fan):
                merged = merged + share(relation, k) * neighbours[k][half]
            pieces.append(merged)
    inputs = jnp.concatenate([piece.astype(BF16) for piece in pieces], axis=1)
    return jnp.dot(inputs, weights, preferred_element_type=F32)


def model_kernel(
    counts, stride, split, slot_hbm, got_hbm, first_hbm, second_hbm, share1_hbm, share2_hbm, mask_hbm,
    loss_ref, sums_ref, slot_ref, got, first_ref, second_ref, share1_ref, share2_ref, mask_ref, wide, x0, x1, x2, h_low, h_high, sems,
    got_sems,
):
    devices, held, _ = got_hbm.shape
    seeds, firsts, _ = counts

    bounds = ((0, split), (split, held))

    def arrive(half):
        span = pl.ds(bounds[half][0], bounds[half][1] - bounds[half][0])
        return pltpu.make_async_copy(got_hbm.at[:, span], got.at[:, span], got_sems.at[half])

    side = [
        pltpu.make_async_copy(source, target, sems.at[number])
        for number, (source, target) in enumerate(
            (
                (slot_hbm, slot_ref), (first_hbm, first_ref), (share2_hbm, share2_ref),
                (share1_hbm, share1_ref), (second_hbm, second_ref), (mask_hbm, mask_ref),
            )
        )
    ]
    side[0].start()
    for half in range(2):
        arrive(half).start()
    for copy in side[1:]:
        copy.start()

    def take(half):
        arrive(half).wait()
        start, end = bounds[half]

        def widen(device, _):
            base = pl.multiple_of(device * stride, 8) + start
            wide[pl.ds(pl.multiple_of(base, 8), end - start), :] = got[
                device, start:end, :
            ].astype(F32)
            return 0

        lax.fori_loop(0, devices, widen, 0)

    side[0].wait()
    take(0)
    firsts_block = -(-seeds // LANES)
    seconds_block = firsts_block + -(-firsts // LANES)

    def fetch(target, block, start, end):
        for item in range(start, end):
            slot = pl.multiple_of(slot_ref[block + item // LANES, item % LANES], 2)
            target[pl.ds(2 * item, 2), :] = wide[pl.ds(slot, 2), :]

    step = HOP_STEP
    fetch(x0, 0, 0, seeds)
    fetch(x1, firsts_block, 0, firsts)
    take(1)
    for number in range(1, len(side)):
        side[number].wait()

    for base in range(0, firsts, step):
        fetch(x2, seconds_block, FAN2 * base, FAN2 * (base + step))
        selves = [x1[pl.ds(2 * base + half, step, stride=2), :] for half in range(2)]
        neighbours = [
            [x2[pl.ds(2 * FAN2 * base + 2 * k + half, step, stride=2 * FAN2), :] for half in range(2)]
            for k in range(FAN2)
        ]
        shares2 = share2_ref[base : base + step, :]
        hidden = layer(
            selves, neighbours,
            lambda r, k, shares2=shares2: shares2[:, r * FAN2 + k : r * FAN2 + k + 1],
            first_ref[...],
        )
        hidden = jnp.maximum(hidden, 0.0).astype(BF16).astype(F32)
        h_low[base : base + step, :] = hidden[:, :LANES]
        h_high[base : base + step, :] = hidden[:, LANES:]

    shares = share1_ref[...]
    share = lambda r, k: shares[:, r * FAN1 + k : r * FAN1 + k + 1]
    selves = [x0[pl.ds(half, seeds, stride=2), :] for half in range(2)]
    neighbours = [
        [x1[pl.ds(2 * k + half, seeds, stride=2 * FAN1), :] for half in range(2)] for k in range(FAN1)
    ]
    hidden = jnp.maximum(layer(selves, neighbours, share, first_ref[...]), 0.0).astype(BF16)
    selves = [hidden[:, :LANES], hidden[:, LANES:]]
    neighbours = [
        [h[pl.ds(k, seeds, stride=FAN1), :] for h in (h_low, h_high)] for k in range(FAN1)
    ]
    second = layer(selves, neighbours, share, second_ref[...])
    positives = mask_ref.shape[1]
    width = second.shape[1]
    contract = (((1,), (1,)), ((), ()))
    loss_sum = jnp.zeros((1, 1), F32)
    for number in range(positives // BLOCK):
        span = slice(number * BLOCK, (number + 1) * BLOCK)
        sources = second[span]
        targets = second[positives + number * BLOCK : positives + (number + 1) * BLOCK]
        negatives = second[2 * positives + number * NEG : 2 * positives + (number + 1) * NEG]
        positive = lax.dot_general(
            jnp.ones((8, width), F32), sources * targets, contract, precision=HIGHEST,
            preferred_element_type=F32,
        )[:1]
        negative = lax.dot_general(
            negatives, sources, contract, precision=HIGHEST, preferred_element_type=F32
        )
        top = jnp.maximum(jnp.max(negative, axis=0, keepdims=True), positive)
        spread = jnp.sum(jnp.exp(negative - top), axis=0, keepdims=True) + jnp.exp(positive - top)
        loss = top + jnp.log(spread) - positive
        loss_ref[:, span] = loss
        loss_sum = loss_sum + jnp.sum(
            mask_ref[:, span].astype(F32) * loss, axis=1, keepdims=True
        )
    edge_sum = jnp.sum(mask_ref[...].astype(F32), axis=1, keepdims=True)
    lane = lax.broadcasted_iota(jnp.int32, (devices, 1, LANES), 2)
    sums_ref[...] = jnp.where(
        lane == 0, loss_sum.reshape(1, 1, 1), jnp.where(lane == 1, edge_sum.reshape(1, 1, 1), 0.0)
    )


def mean_kernel(sums_ref, mean_ref):
    totals = jnp.sum(sums_ref[...], axis=0)
    mean_ref[...] = totals[:, :1] / jnp.maximum(totals[:, 1:2], 1.0)


def mean_shares(relations):
    onehot = (relations[..., None] == jnp.arange(R, dtype=jnp.int32)).astype(F32)
    tallies = jnp.maximum(jnp.sum(onehot, axis=1), 1.0)
    shares = onehot / tallies[:, None, :]
    return jnp.transpose(shares, (0, 2, 1)).reshape(relations.shape[0], -1)


def exchange(array):
    return lax.all_to_all(array, "dom", split_axis=0, concat_axis=0, tiled=True)


def shards(
    features, w_first, w_second, seed_owner, seed_row, hop1_owner, hop1_row, hop1_rel,
    hop2_owner, hop2_row, hop2_rel, edge_mask,
):
    devices = lax.axis_size("dom")
    nodes, width = features.shape
    owners = (seed_owner, hop1_owner, hop2_owner)
    rows = (seed_row, hop1_row, hop2_row)
    counts = tuple(row.shape[0] for row in rows)
    capacities = [(2 * count + devices - 1) // devices for count in counts]
    offsets = [sum(capacities[:kind]) for kind in range(len(counts))]
    slots = sum(capacities)
    held = 2 * slots
    stride = round_up(held, 8)
    blocks = sum(-(-count // LANES) for count in counts)

    requests, places = pl.pallas_call(
        functools.partial(bucket_kernel, offsets, stride, counts),
        out_shape=(
            pltpu.VMEM((devices, 1, round_up(slots, LANES)), jnp.int32),
            pltpu.VMEM((blocks, LANES), jnp.int32),
        ),
        in_specs=[full()] * 6,
        out_specs=(full(), full()),
        scratch_shapes=[
            pltpu.VMEM((blocks * devices, LANES), BF16),
            pltpu.VMEM((blocks * devices, 2 * LANES), F32),
            pltpu.VMEM((2 * devices, blocks * LANES), BF16),
            pltpu.VMEM((round_up(slots, LANES), blocks * LANES), BF16),
        ],
        name="bucket",
    )(*[owner.reshape(1, -1) for owner in owners], *rows)

    arrived = exchange(requests)
    chunk = nodes // 16
    group = devices // PARTS
    located = pl.pallas_call(
        functools.partial(gather_kernel, slots, chunk, group),
        out_shape=jax.ShapeDtypeStruct((devices, held, LANES), BF16),
        in_specs=[full(pl.ANY), full(pl.ANY)],
        out_specs=full(pl.ANY),
        scratch_shapes=[
            pltpu.SMEM(arrived.shape, jnp.int32),
            pltpu.VMEM((nodes, width), BF16),
            pltpu.VMEM((2 * nodes, LANES), F32),
            pltpu.VMEM((2, stride, LANES), F32),
            pltpu.VMEM((devices, held, LANES), BF16),
            pltpu.SemaphoreType.DMA,
            pltpu.SemaphoreType.DMA((nodes // chunk,)),
            pltpu.SemaphoreType.DMA((PARTS,)),
        ],
        name="owner_gather",
    )(arrived, features)
    returned = exchange(located)

    share1 = mean_shares(hop1_rel.reshape(counts[0], FAN1))
    share2 = mean_shares(hop2_rel.reshape(counts[1], FAN2))
    positives = edge_mask.shape[0]
    loss, sums = pl.pallas_call(
        functools.partial(model_kernel, counts, stride, round_up(2 * offsets[2], 8)),
        out_shape=(
            pltpu.VMEM((1, positives), F32),
            pltpu.VMEM((devices, 1, LANES), F32),
        ),
        in_specs=[full(pl.ANY)] * 7,
        out_specs=(full(), full()),
        scratch_shapes=[
            pltpu.SMEM((blocks, LANES), jnp.int32),
            pltpu.VMEM((devices, held, LANES), BF16),
            pltpu.VMEM(w_first.shape, BF16),
            pltpu.VMEM(w_second.shape, BF16),
            pltpu.VMEM(share1.shape, F32),
            pltpu.VMEM(share2.shape, F32),
            pltpu.VMEM((1, positives), jnp.int32),
            pltpu.VMEM((devices * stride, LANES), F32),
        ]
        + [pltpu.VMEM((2 * count, LANES), F32) for count in counts]
        + [pltpu.VMEM((counts[1], LANES), F32)] * 2
        + [pltpu.SemaphoreType.DMA((6,)), pltpu.SemaphoreType.DMA((2,))],
        name="model",
    )(places, returned, w_first, w_second, share1, share2, edge_mask.reshape(1, -1))
    mean_loss = pl.pallas_call(
        mean_kernel,
        out_shape=jax.ShapeDtypeStruct((1, 1), F32),
        in_specs=[full()],
        out_specs=full(),
        compiler_params=pltpu.CompilerParams(vmem_limit_bytes=2**20),
        name="mean",
    )(exchange(sums))
    return (loss.reshape(positives), mean_loss.reshape(()))


def solution(mesh):
    placed = (
        P("dom", None), P(), P(), P("dom", None), P("dom"), P("dom", None), P("dom"), P("dom"),
        P("dom", None), P("dom"), P("dom"), P("dom"),
    )
    return jax.shard_map(
        shards, mesh=mesh, in_specs=placed, out_specs=(P("dom"), P()), check_vma=False
    )
```
